512 devices in a mesh: row: 32 (over y, x, core), col: 16 (over z).
Axes of the slice: x: 4, y: 4, z: 16, core: 2. Of those that a mesh axis runs over, the one named last changes fastest.
Arguments:
- positions: float32 [3, 262144], P(None, ('row', 'col')), may hold values from -6 to 6
- velocities: float32 [3, 262144], P(None, ('row', 'col')), may hold values from -6 to 6
- accels: float32 [3, 262144], P(None, ('row', 'col')), may hold values from -0.75 to 0.75
- jerks: float32 [3, 262144], P(None, ('row', 'col')), may hold values from -1.5 to 1.5
- masses: float32 [262144], P(('row', 'col')), may hold values from 0.3 to 3
- elapsed: float32 [262144], P(('row', 'col')), may hold values from 0.05 to 0.5
- active_star: int32 [4096], replicated, may hold values from 0 to 262143, as said below
Outputs:
- new_positions: float32 [3, 262144], P(None, ('row', 'col'))
- new_velocities: float32 [3, 262144], P(None, ('row', 'col'))
- new_accels: float32 [3, 262144], P(None, ('row', 'col'))
- new_jerks: float32 [3, 262144], P(None, ('row', 'col'))
The draws below stay inside these ranges and needn't reach their ends.
Inputs may be any that keep to these rules, and one draw needn't show every extreme that they name: `active_star`: the 4096 ids are distinct. Star g is owned by device g // 512, devices counted with row slowest and col fastest. In each aligned block of 128 entries (one group of targets), at most 12 entries name stars whose owning device has the same col index, and in every block some col index has exactly 12.
All inputs are finite; a program needn't handle non-finite values.
Results may differ from the reference program's by a relative error of at most 0.0003.
Values sent between devices are 32-bit elements; how exact they have to be, the bound alone decides.
A program may use at most 64 MiB of HBM per device.

```python
import math
import jax
import jax.numpy as jnp
from jax import lax

STAR_DEV = 512
I_DEV = 128
CAP = 12
NSTARS = 262144
ACTIVE = 4096


def clump_layout(key):
    clump_count = max(NSTARS // 512, 4)
    layout_key = jax.random.fold_in(key, 7001)
    key_member, key_centre, key_width, key_drift = jax.random.split(layout_key, 4)
    member = jax.random.randint(key_member, (NSTARS,), 0, clump_count)
    centres = jax.random.normal(key_centre, (3, clump_count), jnp.float32)
    log_width = jax.random.uniform(key_width, (clump_count,), jnp.float32, jnp.log(0.04), jnp.log(0.12))
    drift_speed = 0.4 * jax.random.normal(key_drift, (3, clump_count), jnp.float32)
    return (member, centres, jnp.exp(log_width), drift_speed)


def draw_positions(key, part):
    member, centres, widths, drift_speed = clump_layout(key)
    offsets = jax.random.normal(jax.random.fold_in(key, 7002), (3, NSTARS), jnp.float32)
    placed = jnp.take(centres, member, axis=1) + jnp.take(widths, member)[None, :] * offsets
    return jnp.clip(placed, -6.0, 6.0).astype(jnp.float32)


def draw_velocities(key, part):
    member, centres, widths, drift_speed = clump_layout(key)
    inner_key = jax.random.fold_in(key, 7003)
    scatter = 0.3 * jax.random.normal(inner_key, (3, NSTARS), jnp.float32)
    moving = jnp.take(drift_speed, member, axis=1) + scatter
    return jnp.clip(moving, -6.0, 6.0).astype(jnp.float32)


def draw_active_star(key, part):
    rows_axis = ACTIVE // I_DEV
    cols_axis = NSTARS // (STAR_DEV * rows_axis)
    slots_all = cols_axis * CAP
    first_key, second_key = jax.random.split(key)

    def choose(subkey):
        key_full, key_score, key_order = jax.random.split(subkey, 3)
        forced = jax.random.randint(key_full, (), 0, cols_axis)
        serial = jnp.arange(slots_all, dtype=jnp.int32)
        scores = jax.random.randint(key_score, (slots_all,), 0, 1 << 20) * slots_all + serial
        scores = jnp.where(serial // CAP == forced, serial - slots_all, scores)
        chosen = jnp.argsort(scores, stable=True)[:I_DEV]
        return chosen[jax.random.permutation(key_order, I_DEV)]
    picked = jax.vmap(choose)(jax.random.split(first_key, rows_axis))
    column = picked // CAP
    within = picked % CAP
    blockno = jnp.arange(rows_axis, dtype=jnp.int32)[:, None]
    orders = jax.vmap(lambda subkey: jax.random.permutation(subkey, rows_axis * STAR_DEV))(jax.random.split(second_key, cols_axis))
    position = orders[column, blockno * CAP + within]
    owner_row = position // STAR_DEV
    return ((owner_row * cols_axis + column) * STAR_DEV + position % STAR_DEV).reshape(-1).astype(jnp.int32)


def level_of(rng, shape, cuts, low, top_value):
    def one(dim, shards_of):
        draws = jax.random.uniform(jax.random.fold_in(jax.random.fold_in(rng, 6), dim), (shards_of,), jnp.float32, low / len(cuts), top_value / len(cuts))
        return jnp.repeat(jnp.exp(draws), shape[dim] // shards_of).reshape((-1,) + (1,) * (len(shape) - dim - 1))

    factor_of = one(*cuts[0])
    for cut in cuts[1:]:
        factor_of = factor_of * one(*cut)
    return factor_of


def scatter_about(own_key, extent, scale, most, cuts=(), kind=jnp.bfloat16):
    entries = jax.random.normal(own_key, extent, jnp.float32) * scale
    if len(cuts) > 0:
        entries = level_of(own_key, extent, cuts, -0.22, 0.18) * entries
    return jnp.clip(entries, min=-most, max=most).astype(kind)


def setup_inputs(seed: int = 0) -> dict:
    keys = jax.random.split(jax.random.key(seed), 8)
    positions = draw_positions(jax.random.fold_in(keys[7], 71), 0)
    velocities = draw_velocities(jax.random.fold_in(keys[7], 71), 0)
    accels = scatter_about(keys[2], (3, NSTARS), 0.05, 0.75, ((1, 512),), jnp.float32)
    jerks = scatter_about(keys[3], (3, NSTARS), 0.1, 1.5, ((1, 512),), jnp.float32)
    masses = jnp.clip(jnp.exp(math.log(3.0) - 2.3025851 * jax.random.uniform(keys[4], (NSTARS,), jnp.float32) ** level_of(keys[4], (NSTARS,), ((0, 512),), -0.2, 0.2)), 0.3, 3.0)
    elapsed = jnp.clip(jnp.exp(math.log(0.5) - 2.3025851 * jax.random.uniform(keys[5], (NSTARS,), jnp.float32) ** level_of(keys[5], (NSTARS,), ((0, 512),), -0.2, 0.2)), 0.05, 0.5)
    active_star = draw_active_star(jax.random.fold_in(keys[7], 71), 0)
    return dict(positions=positions, velocities=velocities, accels=accels, jerks=jerks, masses=masses, elapsed=elapsed, active_star=active_star)


softening = 0.001

def predict(positions, velocities, accels, jerks, elapsed):
    timestep = elapsed[None, :]
    moved_pos = positions + timestep * (velocities + timestep * (0.5 * accels + timestep * jerks / 6.0))
    moved_vel = velocities + timestep * (accels + 0.5 * timestep * jerks)
    return (moved_pos, moved_vel)

def correct(old_pos, old_vel, old_acc, old_jerk, new_acc, new_jerk, timestep):
    halfstep = 0.5 * timestep
    twelfth = timestep * timestep / 12.0
    new_vel = old_vel + halfstep * (old_acc + new_acc) + twelfth * (old_jerk - new_jerk)
    new_pos = old_pos + halfstep * (old_vel + new_vel) + twelfth * (old_acc - new_acc)
    return (new_pos, new_vel)

def pair_sums(targets, sources, ceiling):
    jcount = sources.shape[1]
    blk_width = math.gcd(jcount, ceiling)
    jpieces = jnp.transpose(sources.reshape(7, jcount // blk_width, blk_width), (1, 0, 2))

    def advance(running, jpiece):
        separation = jpiece[0:3, None, :] - targets[0:3, :, None]
        rel_velocity = jpiece[3:6, None, :] - targets[3:6, :, None]
        radius_sq = lax.optimization_barrier(jnp.sum(separation * separation, axis=0)) + softening
        inverse = lax.rsqrt(radius_sq)
        weight = jpiece[6][None, :] * inverse * inverse * inverse
        closing = 3.0 * lax.optimization_barrier(jnp.sum(separation * rel_velocity, axis=0)) / radius_sq
        accel_sum = lax.optimization_barrier(jnp.sum(weight[None] * separation, axis=2))
        change = lax.optimization_barrier(jnp.sum(weight[None] * (rel_velocity - closing[None] * separation), axis=2))
        return (running + jnp.concatenate([accel_sum, change], axis=0), None)
    initial = jnp.zeros((6, targets.shape[1]), jnp.float32)
    summed, unused = lax.scan(advance, initial, jpieces)
    return summed

def reference(positions, velocities, accels, jerks, masses, elapsed, active_star):
    moved_pos, moved_vel = predict(positions, velocities, accels, jerks, elapsed)
    sources = jnp.concatenate([moved_pos, moved_vel, masses[None, :]], axis=0)
    targets = jnp.take(sources[0:6], active_star, axis=1)
    summed = pair_sums(targets, sources, 2048) * (1.0 / NSTARS)
    new_acc = summed[0:3]
    new_jerk = summed[3:6]
    timestep = jnp.take(elapsed, active_star)[None, :]
    new_pos, new_vel = correct(jnp.take(positions, active_star, axis=1), jnp.take(velocities, active_star, axis=1), jnp.take(accels, active_star, axis=1), jnp.take(jerks, active_star, axis=1), new_acc, new_jerk, timestep)
    return (positions.at[:, active_star].set(new_pos), velocities.at[:, active_star].set(new_vel), accels.at[:, active_star].set(new_acc), jerks.at[:, active_star].set(new_jerk))
```

```python
import functools

import jax
import jax.numpy as jnp
from jax import lax
from jax.experimental import pallas as pl
from jax.experimental.pallas import tpu as pltpu
from jax.sharding import PartitionSpec as P

softening = 0.001
LANES = 128
MESH = pl.DeviceIdType.MESH


def correct(old_pos, old_vel, old_acc, old_jerk, new_acc, new_jerk, timestep):
    halfstep = 0.5 * timestep
    twelfth = timestep * timestep / 12.0
    new_vel = old_vel + halfstep * (old_acc + new_acc) + twelfth * (old_jerk - new_jerk)
    new_pos = old_pos + halfstep * (old_vel + new_vel) + twelfth * (old_acc - new_acc)
    return (new_pos, new_vel)


def split_moments(block):
    rows = lax.broadcasted_iota(jnp.int32, block.shape, 0)
    weighted = block * jnp.where(rows < 6, block[6:7], 1.0)
    high = weighted.astype(jnp.bfloat16).astype(jnp.float32)
    rest = weighted - high
    middle = rest.astype(jnp.bfloat16).astype(jnp.float32)
    low = rest - middle
    return jnp.concatenate([high, middle, low, jnp.zeros_like(block)], axis=0).astype(jnp.bfloat16)


def weigh_block(srcs, block, tb, wbuf, bbuf, rbuf, slot):
    width = srcs.shape[2]
    moments = split_moments(srcs[block])
    rbuf[slot, :, 0:width] = moments
    rbuf[slot, :, width : 2 * width] = moments
    for chunk in range(width // LANES):
        lanes = pl.ds(chunk * LANES, LANES)
        high = pl.ds(chunk * LANES, LANES)
        low = pl.ds(width + chunk * LANES, LANES)
        source = [
            jnp.broadcast_to(srcs[block, k : k + 1, lanes], (16, LANES)) for k in range(6)
        ]
        for part in range(tb.shape[1] // 16):
            rows = pl.ds(part * 16, 16)
            dx, dy, dz, ux, uy, uz = [source[k] - tb[k, rows, :] for k in range(6)]
            radius_sq = (dx * dx + dy * dy) + (dz * dz + softening)
            inverse = lax.rsqrt(radius_sq)
            inverse_sq = inverse * inverse
            weight = inverse * inverse_sq
            closing = (dx * ux + dy * uy) + dz * uz
            bend = (weight * inverse_sq) * closing
            weight_high = weight.astype(jnp.bfloat16)
            bend_high = bend.astype(jnp.bfloat16)
            wbuf[slot, rows, high] = weight_high
            wbuf[slot, rows, low] = (weight - weight_high.astype(jnp.float32)).astype(jnp.bfloat16)
            bbuf[slot, rows, high] = bend_high
            bbuf[slot, rows, low] = (bend - bend_high.astype(jnp.float32)).astype(jnp.bfloat16)


def add_block(wbuf, bbuf, rbuf, wacc, bacc, slot):
    dims = (((1,), (1,)), ((), ()))
    moments = rbuf[slot]
    wacc[...] += lax.dot_general(wbuf[slot], moments, dims, preferred_element_type=jnp.float32)
    bacc[...] += lax.dot_general(bbuf[slot], moments, dims, preferred_element_type=jnp.float32)


def spread_targets(targets, tb):
    count = targets.shape[1]
    square = jnp.concatenate([targets] * (count // 8), axis=0)
    columns = square.T
    for k in range(6):
        tb[k] = jnp.broadcast_to(columns[:, k : k + 1], (count, LANES))


def pair_sums(srcs, targets, tb, wbuf, bbuf, rbuf, wacc, bacc):
    blocks = srcs.shape[0]
    spread_targets(targets, tb)
    wacc[...] = jnp.zeros_like(wacc)
    bacc[...] = jnp.zeros_like(bacc)
    wbuf[1] = jnp.zeros(wbuf.shape[1:], wbuf.dtype)
    bbuf[1] = jnp.zeros(bbuf.shape[1:], bbuf.dtype)
    rbuf[1] = jnp.zeros(rbuf.shape[1:], rbuf.dtype)

    def advance(j, carry):
        weigh_block(srcs, 2 * j, tb, wbuf, bbuf, rbuf, 0)
        add_block(wbuf, bbuf, rbuf, wacc, bacc, 1)
        weigh_block(srcs, 2 * j + 1, tb, wbuf, bbuf, rbuf, 1)
        add_block(wbuf, bbuf, rbuf, wacc, bacc, 0)
        return carry

    lax.fori_loop(0, blocks // 2, advance, 0)
    add_block(wbuf, bbuf, rbuf, wacc, bacc, 1)

    def folded(total):
        padded = jnp.concatenate([total, jnp.zeros((total.shape[0], LANES - 32), jnp.float32)], axis=1)
        turned = padded.T
        moment = turned[0:8] + turned[8:16] + turned[16:24]
        return moment - targets * moment[6:7]

    direct = folded(wacc[...])
    bent = folded(bacc[...])
    rows = lax.broadcasted_iota(jnp.int32, direct.shape, 0)
    shifted = pltpu.roll(bent, 3, 0)
    both = jnp.where(rows >= 3, direct - 3.0 * shifted, direct)
    return jnp.where(rows < 6, both, 0.0)


def take_lanes(tile, index):
    return jnp.take_along_axis(tile, index, axis=1, mode="promise_in_bounds")


def step_kernel(
    rows_n,
    cols_n,
    pos_h,
    vel_h,
    acc_h,
    jrk_h,
    mass_h,
    ela_h,
    ids_h,
    landed,
    pos,
    vel,
    acc,
    jrk,
    mass,
    ela,
    ids,
    srcs,
    picked,
    near,
    mine,
    far,
    part,
    parts,
    force,
    forces,
    found,
    tb,
    wbuf,
    bbuf,
    rbuf,
    wacc,
    bacc,
    in_sems,
    send_sems,
    recv_sems,
):
    row = lax.axis_index("row")
    col = lax.axis_index("col")
    stars = pos.shape[1]
    slots = stars // LANES
    groups = ids.shape[0]
    scale = 1.0 / (stars * rows_n * cols_n)

    loads = [
        pltpu.make_async_copy(src, dst, in_sems.at[i])
        for i, (src, dst) in enumerate(
            zip((pos_h, vel_h, acc_h, jrk_h, mass_h, ela_h, ids_h), (pos, vel, acc, jrk, mass, ela, ids))
        )
    ]
    for load in loads:
        load.start()

    barrier = pltpu.get_barrier_semaphore()
    for d in range(1, rows_n):
        pl.semaphore_signal(
            barrier, 1, device_id={"row": lax.rem(row + d, rows_n)}, device_id_type=MESH
        )
    for d in range(1, cols_n):
        pl.semaphore_signal(
            barrier, 1, device_id={"col": lax.rem(col + d, cols_n)}, device_id_type=MESH
        )

    for load in loads:
        load.wait()

    t = ela[...]
    p, v, a, j = pos[...], vel[...], acc[...], jrk[...]
    moved_pos = p + t * (v + t * (0.5 * a + t * j / 6.0))
    moved_vel = v + t * (a + 0.5 * t * j)
    own = rows_n - 1
    srcs[own] = jnp.concatenate(
        [moved_pos, moved_vel, mass[...], jnp.zeros((1, stars), jnp.float32)], axis=0
    )

    first = (row * cols_n + col) * stars

    def pick(g, carry):
        local = jnp.broadcast_to(ids[pl.ds(g, 1), :], (8, LANES)) - first
        inside = jnp.logical_and(local >= 0, local < stars)
        lane = jnp.bitwise_and(local, LANES - 1)
        tile = jnp.zeros((8, LANES), jnp.float32)
        for s in range(slots):
            held = jnp.logical_and(local >= s * LANES, local < (s + 1) * LANES)
            tile = jnp.where(held, take_lanes(srcs[own, :, s * LANES : (s + 1) * LANES], lane), tile)
        picked[g] = jnp.where(inside, tile, 0.0)
        return carry

    lax.fori_loop(0, groups, pick, 0, unroll=4)

    pl.semaphore_wait(barrier, rows_n - 1 + cols_n - 1)

    def send(src, dst, sem, axis, peer):
        copy = pltpu.make_async_remote_copy(
            src_ref=src,
            dst_ref=dst,
            send_sem=send_sems.at[sem],
            recv_sem=recv_sems.at[sem],
            device_id={axis: peer},
            device_id_type=MESH,
        )
        copy.start()

    def whole(ref, sem):
        return pltpu.make_async_remote_copy(
            src_ref=ref,
            dst_ref=ref,
            send_sem=send_sems.at[sem],
            recv_sem=recv_sems.at[sem],
            device_id={"row": row},
            device_id_type=MESH,
        )

    for d in range(1, rows_n):
        peer = lax.rem(row + d, rows_n)
        send(picked.at[peer], near.at[d - 1], 0, "row", peer)
    for d in range(1, rows_n):
        peer = lax.rem(row + d, rows_n)
        send(srcs.at[own], srcs.at[d - 1], 1, "row", peer)

    sublane = lax.broadcasted_iota(jnp.int32, (8, LANES), 0)
    lane_f = lax.broadcasted_iota(jnp.int32, (8, LANES), 1).astype(jnp.float32)

    def find(k, carry):
        star = first + k * 8 + sublane
        at = jnp.full((8, LANES), -1.0, jnp.float32)
        for g in range(groups):
            at = jnp.where(jnp.broadcast_to(ids[g : g + 1, :], (8, LANES)) == star, float(g), at)
        found[pl.ds(pl.multiple_of(k * 8, 8), 8), :] = jnp.where(at >= 0.0, at * LANES + lane_f, -1.0)
        return carry

    lax.fori_loop(0, stars // 8, find, 0, unroll=2)
    spots = [
        jnp.max(found[s * LANES : (s + 1) * LANES, :].T, axis=0, keepdims=True) for s in range(slots)
    ]

    whole(near, 0).wait_recv()
    total = picked[row]
    for d in range(rows_n - 1):
        total = total + near[d]
    mine[...] = total
    order = sorted(range(1, cols_n), key=lambda d: -min(d, cols_n - d))
    for d in order:
        send(mine, far.at[d - 1], 2, "col", lax.rem(col + d, cols_n))
    whole(far, 2).wait_recv()
    targets = mine[...]
    for d in range(cols_n - 1):
        targets = targets + far[d]

    whole(srcs.at[pl.ds(0, own)], 1).wait_recv()
    summed = pair_sums(srcs, targets, tb, wbuf, bbuf, rbuf, wacc, bacc)

    part[...] = summed
    for d in order:
        send(part, parts.at[d - 1], 3, "col", lax.rem(col + d, cols_n))
    whole(parts, 3).wait_recv()
    total = part[...]
    for d in range(cols_n - 1):
        total = total + parts[d]
    force[...] = total * scale
    for d in range(1, rows_n):
        send(force, forces.at[d - 1], 4, "row", lax.rem(row + d, rows_n))
    places = []
    for s in range(slots):
        spot = jnp.broadcast_to(spots[s], (8, LANES)).astype(jnp.int32)
        group = lax.shift_right_arithmetic(spot, 7)
        places.append((group, jnp.bitwise_and(spot, LANES - 1)))
    whole(forces, 4).wait_recv()

    top = lax.broadcasted_iota(jnp.int32, (8, LANES), 0)
    for s in range(slots):
        group, lane = places[s]
        out = jnp.where(group == row, take_lanes(force[...], lane), 0.0)
        for d in range(1, rows_n):
            sender = lax.rem(row + rows_n - d, rows_n)
            out = jnp.where(group == sender, take_lanes(forces[d - 1], lane), out)
        flag = jnp.where(group >= 0, 1.0, 0.0)
        landed[:, s * LANES : (s + 1) * LANES] = jnp.where(top == 6, flag, out)

    whole(near, 0).wait_send()
    whole(srcs.at[pl.ds(0, own)], 1).wait_send()
    whole(far, 2).wait_send()
    whole(parts, 3).wait_send()
    whole(forces, 4).wait_send()


def on_device(rows_n, cols_n, positions, velocities, accels, jerks, masses, elapsed, active_star):
    stars = positions.shape[1]
    groups = rows_n
    size = active_star.shape[0] // groups
    f32 = jnp.float32
    tile = (8, LANES)
    landed = pl.pallas_call(
        functools.partial(step_kernel, rows_n, cols_n),
        out_shape=jax.ShapeDtypeStruct((8, stars), f32),
        in_specs=[pl.BlockSpec(memory_space=pl.ANY)] * 7,
        out_specs=pl.BlockSpec(memory_space=pltpu.VMEM),
        scratch_shapes=[
            pltpu.VMEM((3, stars), f32),
            pltpu.VMEM((3, stars), f32),
            pltpu.VMEM((3, stars), f32),
            pltpu.VMEM((3, stars), f32),
            pltpu.VMEM((1, stars), f32),
            pltpu.VMEM((1, stars), f32),
            pltpu.VMEM((groups, size), jnp.int32),
            pltpu.VMEM((rows_n, 8, stars), f32),
            pltpu.VMEM((groups,) + tile, f32),
            pltpu.VMEM((rows_n - 1,) + tile, f32),
            pltpu.VMEM(tile, f32),
            pltpu.VMEM((cols_n - 1,) + tile, f32),
            pltpu.VMEM(tile, f32),
            pltpu.VMEM((cols_n - 1,) + tile, f32),
            pltpu.VMEM(tile, f32),
            pltpu.VMEM((rows_n - 1,) + tile, f32),
            pltpu.VMEM((stars, LANES), f32),
            pltpu.VMEM((6, size, LANES), f32),
            pltpu.VMEM((2, size, 2 * stars), jnp.bfloat16),
            pltpu.VMEM((2, size, 2 * stars), jnp.bfloat16),
            pltpu.VMEM((2, 32, 2 * stars), jnp.bfloat16),
            pltpu.VMEM((size, 32), f32),
            pltpu.VMEM((size, 32), f32),
            pltpu.SemaphoreType.DMA((7,)),
            pltpu.SemaphoreType.DMA((5,)),
            pltpu.SemaphoreType.DMA((5,)),
        ],
        compiler_params=pltpu.CompilerParams(collective_id=0, has_side_effects=True),
        name="block_step",
    )(
        positions,
        velocities,
        accels,
        jerks,
        masses[None, :],
        elapsed[None, :],
        active_star.reshape(groups, size),
    )
    active = landed[6:7] > 0.5
    new_acc = landed[0:3]
    new_jerk = landed[3:6]
    new_pos, new_vel = correct(
        positions, velocities, accels, jerks, new_acc, new_jerk, elapsed[None, :]
    )
    return (
        jnp.where(active, new_pos, positions),
        jnp.where(active, new_vel, velocities),
        jnp.where(active, new_acc, accels),
        jnp.where(active, new_jerk, jerks),
    )


def solution(mesh):
    split = P(None, ("row", "col"))
    flat = P(("row", "col"))
    return jax.shard_map(
        functools.partial(on_device, mesh.shape["row"], mesh.shape["col"]),
        mesh=mesh,
        in_specs=(split, split, split, split, flat, flat, P()),
        out_specs=(split, split, split, split),
        check_vma=False,
    )
```

```python
import functools

import jax
import jax.numpy as jnp
from jax import lax
from jax.experimental import pallas as pl
from jax.experimental.pallas import tpu as pltpu
from jax.sharding import PartitionSpec as P

softening = 0.001
LANES = 128
MESH = pl.DeviceIdType.MESH
ROWS = 16
CAP = 12


def correct(old_pos, old_vel, old_acc, old_jerk, new_acc, new_jerk, timestep):
    halfstep = 0.5 * timestep
    twelfth = timestep * timestep / 12.0
    new_vel = old_vel + halfstep * (old_acc + new_acc) + twelfth * (old_jerk - new_jerk)
    new_pos = old_pos + halfstep * (old_vel + new_vel) + twelfth * (old_acc - new_acc)
    return (new_pos, new_vel)


def split_moments(block):
    zero = jnp.zeros((1, block.shape[1]), jnp.float32)
    block = jnp.concatenate([block, zero], axis=0)
    rows = lax.broadcasted_iota(jnp.int32, block.shape, 0)
    weighted = block * jnp.where(rows < 6, block[6:7], 1.0)
    high = weighted.astype(jnp.bfloat16).astype(jnp.float32)
    rest = weighted - high
    middle = rest.astype(jnp.bfloat16).astype(jnp.float32)
    low = rest - middle
    return jnp.concatenate([high, middle, low, jnp.zeros_like(block)], axis=0).astype(jnp.bfloat16)


def below(value):
    return value - value.astype(jnp.bfloat16).astype(jnp.float32)


def weigh_block(srcs, block, tb, moments, waccs, baccs):
    width = srcs.shape[2]
    moments[0:32, :] = split_moments(srcs[block])
    for tile in range(width // 256):
        at = tile * 256
        for unit in range(2):
            pltpu.matmul_push_rhs(
                moments[:, at : at + 256], staging_register=tile % 2, mxu_index=unit, transpose=True
            )
        source = [
            [
                jnp.broadcast_to(srcs[block, k : k + 1, at + h * LANES : at + (h + 1) * LANES], (ROWS, LANES))
                for k in range(6)
            ]
            for h in range(2)
        ]
        for part in range(len(waccs)):
            rows = pl.ds(part * ROWS, ROWS)
            target = [tb[k, rows, :] for k in range(6)]
            weights, bends = [], []
            for h in range(2):
                dx, dy, dz, ux, uy, uz = [source[h][k] - target[k] for k in range(6)]
                radius_sq = (dx * dx + dy * dy) + (dz * dz + softening)
                inverse = lax.rsqrt(radius_sq)
                inverse_sq = inverse * inverse
                weight = inverse * inverse_sq
                closing = (dx * ux + dy * uy) + dz * uz
                weights.append(weight)
                bends.append((weight * inverse_sq) * closing)
            weight = jnp.concatenate(weights, axis=1)
            bend = jnp.concatenate(bends, axis=1)
            fresh = tile % 2 if part < 2 else None
            pltpu.matmul_acc_lhs(waccs[part], weight, load_staged_rhs=fresh)
            pltpu.matmul_acc_lhs(baccs[part], bend)
            pltpu.matmul_acc_lhs(waccs[part], below(weight))
            pltpu.matmul_acc_lhs(baccs[part], below(bend))


def spread_targets(targets, tb):
    for b, tile in enumerate(targets):
        full = jnp.concatenate([tile, jnp.zeros((2, LANES), jnp.float32)], axis=0)
        columns = jnp.concatenate([full] * (LANES // 8), axis=0).T
        for k in range(6):
            tb[k, b * LANES : (b + 1) * LANES, :] = jnp.broadcast_to(columns[:, k : k + 1], (LANES, LANES))


def folded(accs, target):
    turned = jnp.concatenate([pltpu.matmul_pop(acc)[:, 0:LANES] for acc in accs], axis=0).T
    moment = turned[0:8] + turned[8:16] + turned[16:24]
    return moment[0:6] - target * moment[6:7]


def take_lanes(tile, index):
    return jnp.take_along_axis(tile, index, axis=1, mode="promise_in_bounds")


def turn(rows_of):
    return jnp.concatenate([rows_of] * (LANES // rows_of.shape[0]), axis=0).T


def slot_stars(ids, col, cols_n, stars, blocks):
    groups, size = ids.shape
    each = LANES // groups
    turned = turn(ids[...].astype(jnp.float32)).astype(jnp.int32)
    here = jnp.bitwise_and(lax.shift_right_arithmetic(turned, stars.bit_length() - 1), cols_n - 1) == col
    count = jnp.where(here, 1.0, 0.0)
    sub = lax.broadcasted_iota(jnp.int32, (8, LANES), 0)
    before = jnp.zeros((1, LANES), jnp.float32)
    ranks = []
    for i in range(size // 8):
        run = count[i * 8 : (i + 1) * 8]
        for step in (1, 2, 4):
            run = run + jnp.where(sub >= step, pltpu.roll(run, step, 0), 0.0)
        ranks.append(run + before - count[i * 8 : (i + 1) * 8])
        before = before + run[7:8]
    rank = jnp.where(here, jnp.concatenate(ranks, axis=0), -1.0)
    lane = lax.broadcasted_iota(jnp.int32, (1, LANES), 1)
    which = lax.shift_right_arithmetic(lane, groups.bit_length() - 1).astype(jnp.float32)
    found = []
    for b in range(blocks):
        hit = rank == which + float(b * each)
        found.append(jnp.sum(jnp.where(hit, turned + 1, 0), axis=0, keepdims=True) - 1)
    return found


def step_kernel(
    rows_n,
    cols_n,
    pos_h,
    vel_h,
    acc_h,
    jrk_h,
    mass_h,
    ela_h,
    ids_h,
    out_acc,
    out_jerk,
    out_flag,
    pos,
    vel,
    acc,
    jrk,
    mass,
    ela,
    ids,
    srcs,
    picked,
    near,
    part,
    parts,
    found,
    tb,
    moments,
    in_sems,
    send_sems,
    recv_sems,
    src_send,
    src_recv,
    *accs,
):
    row = lax.axis_index("row")
    col = lax.axis_index("col")
    stars = pos.shape[1]
    star_tiles = stars // LANES
    blocks = picked.shape[0]
    scale = 1.0 / (stars * rows_n * cols_n)
    waccs, baccs = accs[0::2], accs[1::2]

    loads = [
        pltpu.make_async_copy(src, dst, in_sems.at[i])
        for i, (src, dst) in enumerate(
            zip((ids_h, pos_h, vel_h, acc_h, jrk_h, mass_h, ela_h), (ids, pos, vel, acc, jrk, mass, ela))
        )
    ]
    for load in loads:
        load.start()

    barrier = pltpu.get_barrier_semaphore()
    for d in range(1, rows_n):
        pl.semaphore_signal(
            barrier, 1, device_id={"row": lax.rem(row + d, rows_n)}, device_id_type=MESH
        )
    for d in range(1, cols_n):
        pl.semaphore_signal(
            barrier, 1, device_id={"col": lax.rem(col + d, cols_n)}, device_id_type=MESH
        )

    loads[0].wait()
    slots = slot_stars(ids, col, cols_n, stars, blocks)
    for load in loads[1:]:
        load.wait()

    t = ela[...]
    p, v, a, j = pos[...], vel[...], acc[...], jrk[...]
    moved_pos = p + t * (v + t * (0.5 * a + t * j / 6.0))
    moved_vel = v + t * (a + 0.5 * t * j)
    own = jnp.concatenate([moved_pos, moved_vel, mass[...]], axis=0)
    srcs[0] = own
    padded = jnp.concatenate([own, jnp.zeros((1, stars), jnp.float32)], axis=0)

    first = (row * cols_n + col) * stars
    mine = []
    for b in range(blocks):
        local = jnp.broadcast_to(slots[b], (8, LANES)) - first
        lane = jnp.bitwise_and(local, LANES - 1)
        tile = jnp.zeros((8, LANES), jnp.float32)
        for s in range(star_tiles):
            held = jnp.logical_and(local >= s * LANES, local < (s + 1) * LANES)
            tile = jnp.where(held, take_lanes(padded[:, s * LANES : (s + 1) * LANES], lane), tile)
        mine.append(tile[0:6])
        picked[b] = tile[0:6]

    pl.semaphore_wait(barrier, rows_n - 1 + cols_n - 1)

    def send(src, dst, send_sem, recv_sem, axis, peer):
        pltpu.make_async_remote_copy(
            src_ref=src,
            dst_ref=dst,
            send_sem=send_sem,
            recv_sem=recv_sem,
            device_id={axis: peer},
            device_id_type=MESH,
        ).start()

    def whole(ref, send_sem, recv_sem):
        return pltpu.make_async_remote_copy(
            src_ref=ref,
            dst_ref=ref,
            send_sem=send_sem,
            recv_sem=recv_sem,
            device_id={"row": row},
            device_id_type=MESH,
        )

    for d in range(1, rows_n):
        peer = lax.rem(row + d, rows_n)
        send(picked, near.at[d - 1], send_sems.at[0], recv_sems.at[0], "row", peer)
    order = sorted(range(1, cols_n), key=lambda d: min(d, cols_n - d))
    for i, d in enumerate(order):
        peer = lax.rem(col + d, cols_n)
        send(srcs.at[0], srcs.at[i + 1], src_send.at[0], src_recv.at[i], "col", peer)

    sublane = lax.broadcasted_iota(jnp.int32, (8, LANES), 0)
    lane_f = lax.broadcasted_iota(jnp.int32, (8, LANES), 1).astype(jnp.float32)
    for k in range(stars // 8):
        star = first + k * 8 + sublane
        at = jnp.full((8, LANES), -1.0, jnp.float32)
        for b in range(blocks):
            at = jnp.where(jnp.broadcast_to(slots[b], (8, LANES)) == star, lane_f + float(b * LANES), at)
        found[k * 8 : (k + 1) * 8, :] = at
    spots = [
        jnp.max(found[s * LANES : (s + 1) * LANES, :].T, axis=0, keepdims=True).astype(jnp.int32)
        for s in range(star_tiles)
    ]
    moments[32:256, :] = jnp.zeros((224, stars), jnp.bfloat16)
    for unit_acc in accs:
        pltpu.matmul_pop(unit_acc)

    whole(near, send_sems.at[0], recv_sems.at[0]).wait_recv()
    targets = []
    for b in range(blocks):
        total = mine[b]
        for d in range(rows_n - 1):
            total = total + near[d, b]
        targets.append(total)
    spread_targets(targets, tb)

    def advance(i, carry):
        @pl.when(i > 0)
        def _():
            whole(srcs.at[0], src_send.at[0], src_recv.at[i - 1]).wait_recv()

        weigh_block(srcs, i, tb, moments, waccs, baccs)
        return carry

    lax.fori_loop(0, cols_n, advance, 0)

    each = LANES // ROWS
    summed = []
    for b in range(blocks):
        direct = folded(waccs[b * each : (b + 1) * each], targets[b])
        bent = folded(baccs[b * each : (b + 1) * each], targets[b])
        summed.append(jnp.concatenate([direct[0:3], direct[3:6] - 3.0 * bent[0:3]], axis=0))
        part[b] = summed[b]
    for d in range(1, rows_n):
        peer = lax.rem(row + d, rows_n)
        send(part, parts.at[d - 1], send_sems.at[1], recv_sems.at[1], "row", peer)
    whole(parts, send_sems.at[1], recv_sems.at[1]).wait_recv()
    forces = []
    for b in range(blocks):
        total = summed[b]
        for d in range(rows_n - 1):
            total = total + parts[d, b]
        forces.append(jnp.concatenate([total * scale, jnp.zeros((2, LANES), jnp.float32)], axis=0))

    for s in range(star_tiles):
        spot = jnp.broadcast_to(spots[s], (8, LANES))
        lane = jnp.bitwise_and(spot, LANES - 1)
        out = jnp.zeros((8, LANES), jnp.float32)
        for b in range(blocks):
            held = jnp.logical_and(spot >= b * LANES, spot < (b + 1) * LANES)
            out = jnp.where(held, take_lanes(forces[b], lane), out)
        lanes = slice(s * LANES, (s + 1) * LANES)
        out_acc[:, lanes] = out[0:3]
        out_jerk[:, lanes] = out[3:6]
        out_flag[:, lanes] = jnp.where(spot[0:3] >= 0, 1.0, 0.0)

    whole(near, send_sems.at[0], recv_sems.at[0]).wait_send()
    whole(srcs.at[pl.ds(1, cols_n - 1)], src_send.at[0], src_recv.at[0]).wait_send()
    whole(parts, send_sems.at[1], recv_sems.at[1]).wait_send()


def on_device(rows_n, cols_n, cap, positions, velocities, accels, jerks, masses, elapsed, active_star):
    stars = positions.shape[1]
    groups = rows_n
    size = active_star.shape[0] // groups
    blocks = cap * groups // LANES
    units = blocks * LANES // ROWS
    f32 = jnp.float32
    tiles = (blocks, 6, LANES)

    def kernel(*refs):
        accs = [pltpu.ACC((i // 2) % 2)((ROWS, 256), f32) for i in range(2 * units)]
        pl.run_scoped(functools.partial(step_kernel, rows_n, cols_n, *refs), *accs)

    shape = jax.ShapeDtypeStruct((3, stars), f32)
    new_acc, new_jerk, flag = pl.pallas_call(
        kernel,
        out_shape=(shape, shape, shape),
        in_specs=[pl.BlockSpec(memory_space=pltpu.HBM)] * 7,
        out_specs=(pl.BlockSpec(memory_space=pltpu.VMEM),) * 3,
        scratch_shapes=[
            pltpu.VMEM((3, stars), f32),
            pltpu.VMEM((3, stars), f32),
            pltpu.VMEM((3, stars), f32),
            pltpu.VMEM((3, stars), f32),
            pltpu.VMEM((1, stars), f32),
            pltpu.VMEM((1, stars), f32),
            pltpu.VMEM((groups, size), jnp.int32),
            pltpu.VMEM((cols_n, 7, stars), f32),
            pltpu.VMEM(tiles, f32),
            pltpu.VMEM((rows_n - 1,) + tiles, f32),
            pltpu.VMEM(tiles, f32),
            pltpu.VMEM((rows_n - 1,) + tiles, f32),
            pltpu.VMEM((stars, LANES), f32),
            pltpu.VMEM((6, blocks * LANES, LANES), f32),
            pltpu.VMEM((256, stars), jnp.bfloat16),
            pltpu.SemaphoreType.DMA((7,)),
            pltpu.SemaphoreType.DMA((2,)),
            pltpu.SemaphoreType.DMA((2,)),
            pltpu.SemaphoreType.DMA((1,)),
            pltpu.SemaphoreType.DMA((cols_n - 1,)),
        ],
        compiler_params=pltpu.CompilerParams(
            collective_id=0, has_side_effects=True
        ),
        name="block_step",
    )(
        positions,
        velocities,
        accels,
        jerks,
        masses[None, :],
        elapsed[None, :],
        active_star.reshape(groups, size),
    )
    active = flag > 0.5
    new_pos, new_vel = correct(
        positions, velocities, accels, jerks, new_acc, new_jerk, elapsed[None, :]
    )
    return (
        jnp.where(active, new_pos, positions),
        jnp.where(active, new_vel, velocities),
        jnp.where(active, new_acc, accels),
        jnp.where(active, new_jerk, jerks),
    )


def solution(mesh):
    split = P(None, ("row", "col"))
    flat = P(("row", "col"))
    return jax.shard_map(
        functools.partial(on_device, mesh.shape["row"], mesh.shape["col"], CAP),
        mesh=mesh,
        in_specs=(split, split, split, split, flat, flat, P()),
        out_specs=(split, split, split, split),
        check_vma=False,
    )
```

```python
import functools

import jax
import jax.numpy as jnp
from jax import lax
from jax.experimental import pallas as pl
from jax.experimental.pallas import tpu as pltpu
from jax.sharding import PartitionSpec as P

softening = 0.001
LANES = 128
MESH = pl.DeviceIdType.MESH
ROWS = 16
CAP = 12


def correct(old_pos, old_vel, old_acc, old_jerk, new_acc, new_jerk, timestep):
    halfstep = 0.5 * timestep
    twelfth = timestep * timestep / 12.0
    new_vel = old_vel + halfstep * (old_acc + new_acc) + twelfth * (old_jerk - new_jerk)
    new_pos = old_pos + halfstep * (old_vel + new_vel) + twelfth * (old_acc - new_acc)
    return (new_pos, new_vel)


def split_moments(block):
    zero = jnp.zeros((1, block.shape[1]), jnp.float32)
    block = jnp.concatenate([block, zero], axis=0)
    rows = lax.broadcasted_iota(jnp.int32, block.shape, 0)
    weighted = block * jnp.where(rows < 6, block[6:7], 1.0)
    high = weighted.astype(jnp.bfloat16).astype(jnp.float32)
    rest = weighted - high
    middle = rest.astype(jnp.bfloat16).astype(jnp.float32)
    low = rest - middle
    return jnp.concatenate([high, middle, low, jnp.zeros_like(block)], axis=0).astype(jnp.bfloat16)


def below(value):
    return value - value.astype(jnp.bfloat16).astype(jnp.float32)


def weigh_block(srcs, block, tb, moments, waccs, baccs):
    width = srcs.shape[2]
    moments[0:32, :] = split_moments(srcs[block])
    for tile in range(width // 256):
        at = tile * 256
        for unit in range(2):
            pltpu.matmul_push_rhs(
                moments[:, at : at + 256], staging_register=tile % 2, mxu_index=unit, transpose=True
            )
        source = [
            [
                jnp.broadcast_to(srcs[block, k : k + 1, at + h * LANES : at + (h + 1) * LANES], (ROWS, LANES))
                for k in range(6)
            ]
            for h in range(2)
        ]
        for part in range(len(waccs)):
            rows = pl.ds(part * ROWS, ROWS)
            target = [tb[k, rows, :] for k in range(6)]
            weights, bends = [], []
            for h in range(2):
                dx, dy, dz, ux, uy, uz = [source[h][k] - target[k] for k in range(6)]
                radius_sq = (dx * dx + dy * dy) + (dz * dz + softening)
                inverse = lax.rsqrt(radius_sq)
                inverse_sq = inverse * inverse
                weight = inverse * inverse_sq
                closing = (dx * ux + dy * uy) + dz * uz
                weights.append(weight)
                bends.append((weight * inverse_sq) * closing)
            weight = jnp.concatenate(weights, axis=1)
            bend = jnp.concatenate(bends, axis=1)
            fresh = tile % 2 if part < 2 else None
            pltpu.matmul_acc_lhs(waccs[part], weight, load_staged_rhs=fresh)
            pltpu.matmul_acc_lhs(baccs[part], bend)
            pltpu.matmul_acc_lhs(waccs[part], below(weight))
            pltpu.matmul_acc_lhs(baccs[part], below(bend))


def spread_targets(targets, tb):
    for b, tile in enumerate(targets):
        full = jnp.concatenate([tile, jnp.zeros((2, LANES), jnp.float32)], axis=0)
        columns = jnp.concatenate([full] * (LANES // 8), axis=0).T
        for k in range(6):
            tb[k, b * LANES : (b + 1) * LANES, :] = jnp.broadcast_to(columns[:, k : k + 1], (LANES, LANES))


def folded(accs, target):
    turned = jnp.concatenate([pltpu.matmul_pop(acc)[:, 0:LANES] for acc in accs], axis=0).T
    moment = turned[0:8] + turned[8:16] + turned[16:24]
    return moment[0:6] - target * moment[6:7]


def take_lanes(tile, index):
    return jnp.take_along_axis(tile, index, axis=1, mode="promise_in_bounds")


def turn(rows_of):
    return jnp.concatenate([rows_of] * (LANES // rows_of.shape[0]), axis=0).T


def slot_stars(ids, col, cols_n, stars, blocks):
    groups, size = ids.shape
    each = LANES // groups
    turned = turn(ids[...].astype(jnp.float32)).astype(jnp.int32)
    here = jnp.bitwise_and(lax.shift_right_arithmetic(turned, stars.bit_length() - 1), cols_n - 1) == col
    count = jnp.where(here, 1.0, 0.0)
    sub = lax.broadcasted_iota(jnp.int32, (8, LANES), 0)
    before = jnp.zeros((1, LANES), jnp.float32)
    ranks = []
    for i in range(size // 8):
        run = count[i * 8 : (i + 1) * 8]
        for step in (1, 2, 4):
            run = run + jnp.where(sub >= step, pltpu.roll(run, step, 0), 0.0)
        ranks.append(run + before - count[i * 8 : (i + 1) * 8])
        before = before + run[7:8]
    rank = jnp.where(here, jnp.concatenate(ranks, axis=0), -1.0)
    lane = lax.broadcasted_iota(jnp.int32, (1, LANES), 1)
    which = lax.shift_right_arithmetic(lane, groups.bit_length() - 1).astype(jnp.float32)
    found = []
    for b in range(blocks):
        hit = rank == which + float(b * each)
        found.append(jnp.sum(jnp.where(hit, turned + 1, 0), axis=0, keepdims=True) - 1)
    return found


def step_kernel(
    rows_n,
    cols_n,
    pos_h,
    vel_h,
    acc_h,
    jrk_h,
    mass_h,
    ela_h,
    ids_h,
    out,
    pos,
    vel,
    acc,
    jrk,
    mass,
    ela,
    ids,
    srcs,
    picked,
    near,
    part,
    parts,
    found,
    tb,
    moments,
    in_sems,
    send_sems,
    recv_sems,
    src_send,
    src_recv,
    told,
    *accs,
):
    row = lax.axis_index("row")
    col = lax.axis_index("col")
    stars = pos.shape[1]
    star_tiles = stars // LANES
    blocks = picked.shape[0]
    scale = 1.0 / (stars * rows_n * cols_n)
    waccs, baccs = accs[0::2], accs[1::2]

    loads = [
        pltpu.make_async_copy(src, dst, in_sems.at[i])
        for i, (src, dst) in enumerate(
            zip((ids_h, pos_h, vel_h, acc_h, jrk_h, mass_h, ela_h), (ids, pos, vel, acc, jrk, mass, ela))
        )
    ]
    for load in loads:
        load.start()

    barrier = pltpu.get_barrier_semaphore()
    core = lax.rem(row, 2)
    mate = row + 1 - 2 * core
    pl.semaphore_signal(barrier, 1, device_id={"row": mate}, device_id_type=MESH)
    for d in range(1, rows_n // 2):
        pl.semaphore_signal(
            barrier, 1, device_id={"row": lax.rem(row - core + 2 * d, rows_n)}, device_id_type=MESH
        )
    for d in range(1, cols_n):
        pl.semaphore_signal(
            barrier,
            1,
            device_id={"row": row - core + 1, "col": lax.rem(col + d, cols_n)},
            device_id_type=MESH,
        )

    loads[0].wait()
    slots = slot_stars(ids, col, cols_n, stars, blocks)
    for load in loads[1:]:
        load.wait()

    t = ela[...]
    p, v, a, j = pos[...], vel[...], acc[...], jrk[...]
    moved_pos = p + t * (v + t * (0.5 * a + t * j / 6.0))
    moved_vel = v + t * (a + 0.5 * t * j)
    own = jnp.concatenate([moved_pos, moved_vel, mass[...]], axis=0)
    srcs[0] = own
    padded = jnp.concatenate([own, jnp.zeros((1, stars), jnp.float32)], axis=0)

    first = (row * cols_n + col) * stars
    mine = []
    for b in range(blocks):
        local = jnp.broadcast_to(slots[b], (8, LANES)) - first
        lane = jnp.bitwise_and(local, LANES - 1)
        tile = jnp.zeros((8, LANES), jnp.float32)
        for s in range(star_tiles):
            held = jnp.logical_and(local >= s * LANES, local < (s + 1) * LANES)
            tile = jnp.where(held, take_lanes(padded[:, s * LANES : (s + 1) * LANES], lane), tile)
        mine.append(tile[0:6])
        picked[b] = tile[0:6]

    def hear(listener, count):
        @pl.when(core == listener)
        def _():
            pl.semaphore_wait(barrier, count)
            pl.semaphore_signal(told, 1, device_id={"row": mate}, device_id_type=MESH)

        @pl.when(core != listener)
        def _():
            pl.semaphore_wait(told, 1)

    hear(0, rows_n - 1)

    def send(src, dst, send_sem, recv_sem, axis, peer):
        pltpu.make_async_remote_copy(
            src_ref=src,
            dst_ref=dst,
            send_sem=send_sem,
            recv_sem=recv_sem,
            device_id={axis: peer},
            device_id_type=MESH,
        ).start()

    def whole(ref, send_sem, recv_sem):
        return pltpu.make_async_remote_copy(
            src_ref=ref,
            dst_ref=ref,
            send_sem=send_sem,
            recv_sem=recv_sem,
            device_id={"row": row},
            device_id_type=MESH,
        )

    for d in range(1, rows_n):
        peer = lax.rem(row + d, rows_n)
        send(picked, near.at[d - 1], send_sems.at[0], recv_sems.at[0], "row", peer)
    hear(1, 2 * cols_n - 1)
    order = sorted(range(1, cols_n), key=lambda d: min(d, cols_n - d))
    for i, d in enumerate(order):
        peer = lax.rem(col + d, cols_n)
        send(srcs.at[0], srcs.at[i + 1], src_send.at[0], src_recv.at[i], "col", peer)

    sublane = lax.broadcasted_iota(jnp.int32, (8, LANES), 0)
    lane_f = lax.broadcasted_iota(jnp.int32, (8, LANES), 1).astype(jnp.float32)
    for k in range(stars // 8):
        star = first + k * 8 + sublane
        at = jnp.full((8, LANES), -1.0, jnp.float32)
        for b in range(blocks):
            at = jnp.where(jnp.broadcast_to(slots[b], (8, LANES)) == star, lane_f + float(b * LANES), at)
        found[k * 8 : (k + 1) * 8, :] = at
    spots = [
        jnp.max(found[s * LANES : (s + 1) * LANES, :].T, axis=0, keepdims=True).astype(jnp.int32)
        for s in range(star_tiles)
    ]
    moments[32:256, :] = jnp.zeros((224, stars), jnp.bfloat16)
    for unit_acc in accs:
        pltpu.matmul_pop(unit_acc)

    whole(near, send_sems.at[0], recv_sems.at[0]).wait_recv()
    targets = []
    for b in range(blocks):
        total = mine[b]
        for d in range(rows_n - 1):
            total = total + near[d, b]
        targets.append(total)
    spread_targets(targets, tb)

    def advance(i, carry):
        @pl.when(i > 0)
        def _():
            whole(srcs.at[0], src_send.at[0], src_recv.at[i - 1]).wait_recv()

        weigh_block(srcs, i, tb, moments, waccs, baccs)
        return carry

    lax.fori_loop(0, cols_n, advance, 0)

    each = LANES // ROWS
    summed = []
    for b in range(blocks):
        direct = folded(waccs[b * each : (b + 1) * each], targets[b])
        bent = folded(baccs[b * each : (b + 1) * each], targets[b])
        summed.append(jnp.concatenate([direct[0:3], direct[3:6] - 3.0 * bent[0:3]], axis=0))
        part[b] = summed[b]
    for d in range(1, rows_n):
        peer = lax.rem(row + d, rows_n)
        send(part, parts.at[d - 1], send_sems.at[1], recv_sems.at[1], "row", peer)
    whole(parts, send_sems.at[1], recv_sems.at[1]).wait_recv()
    forces = []
    for b in range(blocks):
        total = summed[b]
        for d in range(rows_n - 1):
            total = total + parts[d, b]
        forces.append(jnp.concatenate([total * scale, jnp.zeros((2, LANES), jnp.float32)], axis=0))

    for s in range(star_tiles):
        spot = jnp.broadcast_to(spots[s], (8, LANES))
        lane = jnp.bitwise_and(spot, LANES - 1)
        place = jnp.zeros((8, LANES), jnp.float32)
        for b in range(blocks):
            held = jnp.logical_and(spot >= b * LANES, spot < (b + 1) * LANES)
            place = jnp.where(held, take_lanes(forces[b], lane), place)
        lanes = slice(s * LANES, (s + 1) * LANES)
        active = spot[0:3] >= 0
        new_acc, new_jerk = place[0:3], place[3:6]
        new_pos, new_vel = correct(
            pos[:, lanes], vel[:, lanes], acc[:, lanes], jrk[:, lanes], new_acc, new_jerk, ela[:, lanes]
        )
        out[0:3, lanes] = jnp.where(active, new_pos, pos[:, lanes])
        out[4:7, lanes] = jnp.where(active, new_vel, vel[:, lanes])
        out[8:11, lanes] = jnp.where(active, new_acc, acc[:, lanes])
        out[12:15, lanes] = jnp.where(active, new_jerk, jrk[:, lanes])

    whole(near, send_sems.at[0], recv_sems.at[0]).wait_send()
    whole(srcs.at[pl.ds(1, cols_n - 1)], src_send.at[0], src_recv.at[0]).wait_send()
    whole(parts, send_sems.at[1], recv_sems.at[1]).wait_send()


def on_device(rows_n, cols_n, cap, positions, velocities, accels, jerks, masses, elapsed, active_star):
    stars = positions.shape[1]
    groups = rows_n
    size = active_star.shape[0] // groups
    blocks = cap * groups // LANES
    units = blocks * LANES // ROWS
    f32 = jnp.float32
    tiles = (blocks, 6, LANES)

    def kernel(*refs):
        accs = [pltpu.ACC((i // 2) % 2)((ROWS, 256), f32) for i in range(2 * units)]
        pl.run_scoped(functools.partial(step_kernel, rows_n, cols_n, *refs), *accs)

    merged = pl.pallas_call(
        kernel,
        out_shape=jax.ShapeDtypeStruct((16, stars), f32),
        in_specs=[pl.BlockSpec(memory_space=pltpu.HBM)] * 7,
        out_specs=pl.BlockSpec(memory_space=pltpu.VMEM),
        scratch_shapes=[
            pltpu.VMEM((3, stars), f32),
            pltpu.VMEM((3, stars), f32),
            pltpu.VMEM((3, stars), f32),
            pltpu.VMEM((3, stars), f32),
            pltpu.VMEM((1, stars), f32),
            pltpu.VMEM((1, stars), f32),
            pltpu.VMEM((groups, size), jnp.int32),
            pltpu.VMEM((cols_n, 7, stars), f32),
            pltpu.VMEM(tiles, f32),
            pltpu.VMEM((rows_n - 1,) + tiles, f32),
            pltpu.VMEM(tiles, f32),
            pltpu.VMEM((rows_n - 1,) + tiles, f32),
            pltpu.VMEM((stars, LANES), f32),
            pltpu.VMEM((6, blocks * LANES, LANES), f32),
            pltpu.VMEM((256, stars), jnp.bfloat16),
            pltpu.SemaphoreType.DMA((7,)),
            pltpu.SemaphoreType.DMA((2,)),
            pltpu.SemaphoreType.DMA((2,)),
            pltpu.SemaphoreType.DMA((1,)),
            pltpu.SemaphoreType.DMA((cols_n - 1,)),
            pltpu.SemaphoreType.REGULAR,
        ],
        compiler_params=pltpu.CompilerParams(
            collective_id=0, has_side_effects=True
        ),
        name="block_step",
    )(
        positions,
        velocities,
        accels,
        jerks,
        masses[None, :],
        elapsed[None, :],
        active_star.reshape(groups, size),
    )
    return tuple(merged[4 * i : 4 * i + 3] for i in range(4))


def solution(mesh):
    split = P(None, ("row", "col"))
    flat = P(("row", "col"))
    return jax.shard_map(
        functools.partial(on_device, mesh.shape["row"], mesh.shape["col"], CAP),
        mesh=mesh,
        in_specs=(split, split, split, split, flat, flat, P()),
        out_specs=(split, split, split, split),
        check_vma=False,
    )
```

```python
import functools

import jax
import jax.numpy as jnp
from jax import lax
from jax.experimental import pallas as pl
from jax.experimental.pallas import tpu as pltpu
from jax.sharding import PartitionSpec as P

softening = 0.001
LANES = 128
MESH = pl.DeviceIdType.MESH
ROWS = 16
CAP = 12


def correct(old_pos, old_vel, old_acc, old_jerk, new_acc, new_jerk, timestep):
    halfstep = 0.5 * timestep
    twelfth = timestep * timestep / 12.0
    new_vel = old_vel + halfstep * (old_acc + new_acc) + twelfth * (old_jerk - new_jerk)
    new_pos = old_pos + halfstep * (old_vel + new_vel) + twelfth * (old_acc - new_acc)
    return (new_pos, new_vel)


def split_moments(block):
    zero = jnp.zeros((1, block.shape[1]), jnp.float32)
    block = jnp.concatenate([block, zero], axis=0)
    rows = lax.broadcasted_iota(jnp.int32, block.shape, 0)
    weighted = block * jnp.where(rows < 6, block[6:7], 1.0)
    high = weighted.astype(jnp.bfloat16).astype(jnp.float32)
    rest = weighted - high
    middle = rest.astype(jnp.bfloat16).astype(jnp.float32)
    low = rest - middle
    return jnp.concatenate([high, middle, low, jnp.zeros_like(block)], axis=0).astype(jnp.bfloat16)


def below(value):
    return value - value.astype(jnp.bfloat16).astype(jnp.float32)


def weigh_block(srcs, block, tb, moments, waccs, baccs):
    width = srcs.shape[2]
    moments[0:32, :] = split_moments(srcs[block])
    for tile in range(width // 256):
        at = tile * 256
        for unit in range(2):
            pltpu.matmul_push_rhs(
                moments[:, at : at + 256], staging_register=tile % 2, mxu_index=unit, transpose=True
            )
        source = [
            [
                jnp.broadcast_to(srcs[block, k : k + 1, at + h * LANES : at + (h + 1) * LANES], (ROWS, LANES))
                for k in range(6)
            ]
            for h in range(2)
        ]
        for part in range(len(waccs)):
            rows = pl.ds(part * ROWS, ROWS)
            target = [tb[k, rows, :] for k in range(6)]
            weights, bends = [], []
            for h in range(2):
                dx, dy, dz, ux, uy, uz = [source[h][k] - target[k] for k in range(6)]
                radius_sq = (dx * dx + dy * dy) + (dz * dz + softening)
                inverse = lax.rsqrt(radius_sq)
                inverse_sq = inverse * inverse
                weight = inverse * inverse_sq
                closing = (dx * ux + dy * uy) + dz * uz
                weights.append(weight)
                bends.append((weight * inverse_sq) * closing)
            weight = jnp.concatenate(weights, axis=1)
            bend = jnp.concatenate(bends, axis=1)
            fresh = tile % 2 if part < 2 else None
            pltpu.matmul_acc_lhs(waccs[part], weight, load_staged_rhs=fresh)
            pltpu.matmul_acc_lhs(baccs[part], bend)
            pltpu.matmul_acc_lhs(waccs[part], below(weight))
            pltpu.matmul_acc_lhs(baccs[part], below(bend))


def spread_targets(targets, tb):
    for b, tile in enumerate(targets):
        full = jnp.concatenate([tile, jnp.zeros((2, LANES), jnp.float32)], axis=0)
        columns = jnp.concatenate([full] * (LANES // 8), axis=0).T
        for k in range(6):
            tb[k, b * LANES : (b + 1) * LANES, :] = jnp.broadcast_to(columns[:, k : k + 1], (LANES, LANES))


def folded(accs, target):
    turned = jnp.concatenate([pltpu.matmul_pop(acc)[:, 0:LANES] for acc in accs], axis=0).T
    moment = turned[0:8] + turned[8:16] + turned[16:24]
    return moment[0:6] - target * moment[6:7]


def take_lanes(tile, index):
    return jnp.take_along_axis(tile, index, axis=1, mode="promise_in_bounds")


def turn(rows_of):
    return jnp.concatenate([rows_of] * (LANES // rows_of.shape[0]), axis=0).T


def slot_stars(ids, col, cols_n, stars, blocks):
    groups, size = ids.shape
    each = LANES // groups
    turned = turn(ids[...].astype(jnp.float32)).astype(jnp.int32)
    here = jnp.bitwise_and(lax.shift_right_arithmetic(turned, stars.bit_length() - 1), cols_n - 1) == col
    count = jnp.where(here, 1.0, 0.0)
    sub = lax.broadcasted_iota(jnp.int32, (8, LANES), 0)
    before = jnp.zeros((1, LANES), jnp.float32)
    ranks = []
    for i in range(size // 8):
        run = count[i * 8 : (i + 1) * 8]
        for step in (1, 2, 4):
            run = run + jnp.where(sub >= step, pltpu.roll(run, step, 0), 0.0)
        ranks.append(run + before - count[i * 8 : (i + 1) * 8])
        before = before + run[7:8]
    rank = jnp.where(here, jnp.concatenate(ranks, axis=0), -1.0)
    lane = lax.broadcasted_iota(jnp.int32, (1, LANES), 1)
    which = lax.shift_right_arithmetic(lane, groups.bit_length() - 1).astype(jnp.float32)
    found = []
    for b in range(blocks):
        hit = rank == which + float(b * each)
        found.append(jnp.sum(jnp.where(hit, turned + 1, 0), axis=0, keepdims=True) - 1)
    return found


def step_kernel(
    rows_n,
    cols_n,
    pos_h,
    vel_h,
    acc_h,
    jrk_h,
    mass_h,
    ela_h,
    ids_h,
    out,
    pos,
    vel,
    acc,
    jrk,
    mass,
    ela,
    ids,
    srcs,
    picked,
    near,
    part,
    parts,
    found,
    tb,
    moments,
    in_sems,
    send_sems,
    recv_sems,
    src_send,
    src_recv,
    told,
    beyond,
    *accs,
):
    row = lax.axis_index("row")
    col = lax.axis_index("col")
    stars = pos.shape[1]
    star_tiles = stars // LANES
    blocks = picked.shape[0]
    scale = 1.0 / (stars * rows_n * cols_n)
    waccs, baccs = accs[0::2], accs[1::2]

    loads = [
        pltpu.make_async_copy(src, dst, in_sems.at[i])
        for i, (src, dst) in enumerate(
            zip((ids_h, pos_h, vel_h, acc_h, jrk_h, mass_h, ela_h), (ids, pos, vel, acc, jrk, mass, ela))
        )
    ]
    for load in loads:
        load.start()

    barrier = pltpu.get_barrier_semaphore()
    core = lax.rem(row, 2)
    mate = row + 1 - 2 * core
    reach = cols_n // 4
    near_by = [s * d for d in range(1, reach + 1) for s in (1, -1)]
    pl.semaphore_signal(barrier, 1, device_id={"row": mate}, device_id_type=MESH)
    for d in reversed(near_by):
        pl.semaphore_signal(
            barrier,
            1,
            device_id={"row": row - core + 1, "col": lax.rem(col + d + cols_n, cols_n)},
            device_id_type=MESH,
        )
    for d in range(1, rows_n // 2):
        pl.semaphore_signal(
            barrier, 1, device_id={"row": lax.rem(row - core + 2 * d, rows_n)}, device_id_type=MESH
        )

    loads[0].wait()
    slots = slot_stars(ids, col, cols_n, stars, blocks)
    for load in loads[1:]:
        load.wait()

    t = ela[...]
    p, v, a, j = pos[...], vel[...], acc[...], jrk[...]
    moved_pos = p + t * (v + t * (0.5 * a + t * j / 6.0))
    moved_vel = v + t * (a + 0.5 * t * j)
    own = jnp.concatenate([moved_pos, moved_vel, mass[...]], axis=0)
    srcs[0] = own
    padded = jnp.concatenate([own, jnp.zeros((1, stars), jnp.float32)], axis=0)

    first = (row * cols_n + col) * stars
    mine = []
    for b in range(blocks):
        local = jnp.broadcast_to(slots[b], (8, LANES)) - first
        lane = jnp.bitwise_and(local, LANES - 1)
        tile = jnp.zeros((8, LANES), jnp.float32)
        for s in range(star_tiles):
            held = jnp.logical_and(local >= s * LANES, local < (s + 1) * LANES)
            tile = jnp.where(held, take_lanes(padded[:, s * LANES : (s + 1) * LANES], lane), tile)
        mine.append(tile[0:6])
        picked[b] = tile[0:6]

    def tell_mate():
        pl.semaphore_signal(told, 1, device_id={"row": mate}, device_id_type=MESH)

    def hear(listener, count):
        @pl.when(core == listener)
        def _():
            pl.semaphore_wait(barrier, count)
            tell_mate()

        @pl.when(core != listener)
        def _():
            pl.semaphore_wait(told, 1)

    hear(0, rows_n - 1)

    def send(src, dst, send_sem, recv_sem, axis, peer):
        pltpu.make_async_remote_copy(
            src_ref=src,
            dst_ref=dst,
            send_sem=send_sem,
            recv_sem=recv_sem,
            device_id={axis: peer},
            device_id_type=MESH,
        ).start()

    def whole(ref, send_sem, recv_sem):
        return pltpu.make_async_remote_copy(
            src_ref=ref,
            dst_ref=ref,
            send_sem=send_sem,
            recv_sem=recv_sem,
            device_id={"row": row},
            device_id_type=MESH,
        )

    for d in range(1, rows_n):
        peer = lax.rem(row + d, rows_n)
        send(picked, near.at[d - 1], send_sems.at[0], recv_sems.at[0], "row", peer)
    far_off = [s * d for d in range(reach + 1, cols_n // 2 + 1) for s in (1, -1)][:-1]

    def share():
        def give(d):
            slot = 2 * abs(d) - (1 if d > 0 else 0)
            peer = lax.rem(col + d + cols_n, cols_n)
            send(srcs.at[0], srcs.at[slot], src_send.at[0], src_recv.at[slot - 1], "col", peer)

        hear(1, 2 * len(near_by) + 1)

        @pl.when(core == 1)
        def _():
            for side, d in enumerate((reach, -reach)):
                pl.semaphore_signal(
                    beyond.at[side],
                    1,
                    device_id={"col": lax.rem(col + d + cols_n, cols_n)},
                    device_id_type=MESH,
                )

        for d in near_by:
            give(d)

        @pl.when(core == 1)
        def _():
            pl.semaphore_wait(beyond.at[0], 1)
            pl.semaphore_wait(beyond.at[1], 1)
            tell_mate()

        @pl.when(core != 1)
        def _():
            pl.semaphore_wait(told, 1)

        for d in far_off:
            give(d)

    share()

    sublane = lax.broadcasted_iota(jnp.int32, (8, LANES), 0)
    lane_f = lax.broadcasted_iota(jnp.int32, (8, LANES), 1).astype(jnp.float32)
    for k in range(stars // 8):
        star = first + k * 8 + sublane
        at = jnp.full((8, LANES), -1.0, jnp.float32)
        for b in range(blocks):
            at = jnp.where(jnp.broadcast_to(slots[b], (8, LANES)) == star, lane_f + float(b * LANES), at)
        found[k * 8 : (k + 1) * 8, :] = at
    spots = [
        jnp.max(found[s * LANES : (s + 1) * LANES, :].T, axis=0, keepdims=True).astype(jnp.int32)
        for s in range(star_tiles)
    ]
    moments[32:256, :] = jnp.zeros((224, stars), jnp.bfloat16)
    for unit_acc in accs:
        pltpu.matmul_pop(unit_acc)

    whole(near, send_sems.at[0], recv_sems.at[0]).wait_recv()
    targets = []
    for b in range(blocks):
        total = mine[b]
        for d in range(rows_n - 1):
            total = total + near[d, b]
        targets.append(total)
    spread_targets(targets, tb)

    weigh_block(srcs, 0, tb, moments, waccs, baccs)

    def advance(i, carry):
        whole(srcs.at[0], src_send.at[0], src_recv.at[i - 1]).wait_recv()
        weigh_block(srcs, i, tb, moments, waccs, baccs)
        return carry

    lax.fori_loop(1, cols_n, advance, 0)

    each = LANES // ROWS
    summed = []
    for b in range(blocks):
        direct = folded(waccs[b * each : (b + 1) * each], targets[b])
        bent = folded(baccs[b * each : (b + 1) * each], targets[b])
        summed.append(jnp.concatenate([direct[0:3], direct[3:6] - 3.0 * bent[0:3]], axis=0))
        part[b] = summed[b]
    for d in range(1, rows_n):
        peer = lax.rem(row + d, rows_n)
        send(part, parts.at[d - 1], send_sems.at[1], recv_sems.at[1], "row", peer)
    whole(parts, send_sems.at[1], recv_sems.at[1]).wait_recv()
    forces = []
    for b in range(blocks):
        total = summed[b]
        for d in range(rows_n - 1):
            total = total + parts[d, b]
        forces.append(jnp.concatenate([total * scale, jnp.zeros((2, LANES), jnp.float32)], axis=0))

    for s in range(star_tiles):
        spot = jnp.broadcast_to(spots[s], (8, LANES))
        lane = jnp.bitwise_and(spot, LANES - 1)
        place = jnp.zeros((8, LANES), jnp.float32)
        for b in range(blocks):
            held = jnp.logical_and(spot >= b * LANES, spot < (b + 1) * LANES)
            place = jnp.where(held, take_lanes(forces[b], lane), place)
        lanes = slice(s * LANES, (s + 1) * LANES)
        active = spot[0:3] >= 0
        new_acc, new_jerk = place[0:3], place[3:6]
        new_pos, new_vel = correct(
            pos[:, lanes], vel[:, lanes], acc[:, lanes], jrk[:, lanes], new_acc, new_jerk, ela[:, lanes]
        )
        out[0:3, lanes] = jnp.where(active, new_pos, pos[:, lanes])
        out[4:7, lanes] = jnp.where(active, new_vel, vel[:, lanes])
        out[8:11, lanes] = jnp.where(active, new_acc, acc[:, lanes])
        out[12:15, lanes] = jnp.where(active, new_jerk, jrk[:, lanes])

    whole(near, send_sems.at[0], recv_sems.at[0]).wait_send()
    whole(srcs.at[pl.ds(1, cols_n - 1)], src_send.at[0], src_recv.at[0]).wait_send()
    whole(parts, send_sems.at[1], recv_sems.at[1]).wait_send()


def on_device(rows_n, cols_n, cap, positions, velocities, accels, jerks, masses, elapsed, active_star):
    stars = positions.shape[1]
    groups = rows_n
    size = active_star.shape[0] // groups
    blocks = cap * groups // LANES
    units = blocks * LANES // ROWS
    f32 = jnp.float32
    tiles = (blocks, 6, LANES)

    def kernel(*refs):
        accs = [pltpu.ACC((i // 2) % 2)((ROWS, 256), f32) for i in range(2 * units)]
        pl.run_scoped(functools.partial(step_kernel, rows_n, cols_n, *refs), *accs)

    merged = pl.pallas_call(
        kernel,
        out_shape=jax.ShapeDtypeStruct((16, stars), f32),
        in_specs=[pl.BlockSpec(memory_space=pltpu.HBM)] * 7,
        out_specs=pl.BlockSpec(memory_space=pltpu.VMEM),
        scratch_shapes=[
            pltpu.VMEM((3, stars), f32),
            pltpu.VMEM((3, stars), f32),
            pltpu.VMEM((3, stars), f32),
            pltpu.VMEM((3, stars), f32),
            pltpu.VMEM((1, stars), f32),
            pltpu.VMEM((1, stars), f32),
            pltpu.VMEM((groups, size), jnp.int32),
            pltpu.VMEM((cols_n, 7, stars), f32),
            pltpu.VMEM(tiles, f32),
            pltpu.VMEM((rows_n - 1,) + tiles, f32),
            pltpu.VMEM(tiles, f32),
            pltpu.VMEM((rows_n - 1,) + tiles, f32),
            pltpu.VMEM((stars, LANES), f32),
            pltpu.VMEM((6, blocks * LANES, LANES), f32),
            pltpu.VMEM((256, stars), jnp.bfloat16),
            pltpu.SemaphoreType.DMA((7,)),
            pltpu.SemaphoreType.DMA((2,)),
            pltpu.SemaphoreType.DMA((2,)),
            pltpu.SemaphoreType.DMA((1,)),
            pltpu.SemaphoreType.DMA((cols_n - 1,)),
            pltpu.SemaphoreType.REGULAR,
            pltpu.SemaphoreType.REGULAR((2,)),
        ],
        compiler_params=pltpu.CompilerParams(
            collective_id=0, has_side_effects=True
        ),
        name="block_step",
    )(
        positions,
        velocities,
        accels,
        jerks,
        masses[None, :],
        elapsed[None, :],
        active_star.reshape(groups, size),
    )
    return tuple(merged[4 * i : 4 * i + 3] for i in range(4))


def solution(mesh):
    split = P(None, ("row", "col"))
    flat = P(("row", "col"))
    return jax.shard_map(
        functools.partial(on_device, mesh.shape["row"], mesh.shape["col"], CAP),
        mesh=mesh,
        in_specs=(split, split, split, split, flat, flat, P()),
        out_specs=(split, split, split, split),
        check_vma=False,
    )
```

```python
import functools

import jax
import jax.numpy as jnp
from jax import lax
from jax.experimental import pallas as pl
from jax.experimental.pallas import tpu as pltpu
from jax.sharding import PartitionSpec as P

softening = 0.001
LANES = 128
MESH = pl.DeviceIdType.MESH
ROWS = 16
CAP = 12


def correct(old_pos, old_vel, old_acc, old_jerk, new_acc, new_jerk, timestep):
    halfstep = 0.5 * timestep
    twelfth = timestep * timestep / 12.0
    new_vel = old_vel + halfstep * (old_acc + new_acc) + twelfth * (old_jerk - new_jerk)
    new_pos = old_pos + halfstep * (old_vel + new_vel) + twelfth * (old_acc - new_acc)
    return (new_pos, new_vel)


def split_moments(block):
    zero = jnp.zeros((1, block.shape[1]), jnp.float32)
    block = jnp.concatenate([block, zero], axis=0)
    rows = lax.broadcasted_iota(jnp.int32, block.shape, 0)
    weighted = block * jnp.where(rows < 6, block[6:7], 1.0)
    high = weighted.astype(jnp.bfloat16).astype(jnp.float32)
    rest = weighted - high
    middle = rest.astype(jnp.bfloat16).astype(jnp.float32)
    low = rest - middle
    return jnp.concatenate([high, middle, low, jnp.zeros_like(block)], axis=0).astype(jnp.bfloat16)


def below(value):
    return value - value.astype(jnp.bfloat16).astype(jnp.float32)


def weigh_block(srcs, block, tb, moments, waccs, baccs):
    width = srcs.shape[2]
    moments[0:32, :] = split_moments(srcs[block])
    for tile in range(width // 256):
        at = tile * 256
        for unit in range(2):
            pltpu.matmul_push_rhs(
                moments[:, at : at + 256], staging_register=tile % 2, mxu_index=unit, transpose=True
            )
        source = [
            [
                jnp.broadcast_to(srcs[block, k : k + 1, at + h * LANES : at + (h + 1) * LANES], (ROWS, LANES))
                for k in range(6)
            ]
            for h in range(2)
        ]
        for part in range(len(waccs)):
            rows = pl.ds(part * ROWS, ROWS)
            target = [tb[k, rows, :] for k in range(6)]
            weights, bends = [], []
            for h in range(2):
                dx, dy, dz, ux, uy, uz = [source[h][k] - target[k] for k in range(6)]
                radius_sq = (dx * dx + dy * dy) + (dz * dz + softening)
                inverse = lax.rsqrt(radius_sq)
                inverse_sq = inverse * inverse
                weight = inverse * inverse_sq
                closing = (dx * ux + dy * uy) + dz * uz
                weights.append(weight)
                bends.append((weight * inverse_sq) * closing)
            weight = jnp.concatenate(weights, axis=1)
            bend = jnp.concatenate(bends, axis=1)
            fresh = tile % 2 if part < 2 else None
            pltpu.matmul_acc_lhs(waccs[part], weight, load_staged_rhs=fresh)
            pltpu.matmul_acc_lhs(baccs[part], bend)
            pltpu.matmul_acc_lhs(waccs[part], below(weight))
            pltpu.matmul_acc_lhs(baccs[part], below(bend))


def spread_targets(targets, tb):
    for b, tile in enumerate(targets):
        full = jnp.concatenate([tile, jnp.zeros((2, LANES), jnp.float32)], axis=0)
        columns = jnp.concatenate([full] * (LANES // 8), axis=0).T
        for k in range(6):
            tb[k, b * LANES : (b + 1) * LANES, :] = jnp.broadcast_to(columns[:, k : k + 1], (LANES, LANES))


def folded(accs, target):
    turned = jnp.concatenate([pltpu.matmul_pop(acc)[:, 0:LANES] for acc in accs], axis=0).T
    moment = turned[0:8] + turned[8:16] + turned[16:24]
    return moment[0:6] - target * moment[6:7]


def take_lanes(tile, index):
    return jnp.take_along_axis(tile, index, axis=1, mode="promise_in_bounds")


def turn(rows_of):
    return jnp.concatenate([rows_of] * (LANES // rows_of.shape[0]), axis=0).T


def slot_stars(ids, col, cols_n, stars, blocks):
    groups, size = ids.shape
    each = LANES // groups
    turned = turn(ids[...].astype(jnp.float32)).astype(jnp.int32)
    here = jnp.bitwise_and(lax.shift_right_arithmetic(turned, stars.bit_length() - 1), cols_n - 1) == col
    count = jnp.where(here, 1.0, 0.0)
    sub = lax.broadcasted_iota(jnp.int32, (8, LANES), 0)
    before = jnp.zeros((1, LANES), jnp.float32)
    ranks = []
    for i in range(size // 8):
        run = count[i * 8 : (i + 1) * 8]
        for step in (1, 2, 4):
            run = run + jnp.where(sub >= step, pltpu.roll(run, step, 0), 0.0)
        ranks.append(run + before - count[i * 8 : (i + 1) * 8])
        before = before + run[7:8]
    rank = jnp.where(here, jnp.concatenate(ranks, axis=0), -1.0)
    lane = lax.broadcasted_iota(jnp.int32, (1, LANES), 1)
    which = lax.shift_right_arithmetic(lane, groups.bit_length() - 1).astype(jnp.float32)
    found = []
    for b in range(blocks):
        hit = rank == which + float(b * each)
        found.append(jnp.sum(jnp.where(hit, turned + 1, 0), axis=0, keepdims=True) - 1)
    return found


def step_kernel(
    rows_n,
    cols_n,
    pos_h,
    vel_h,
    acc_h,
    jrk_h,
    mass_h,
    ela_h,
    ids_h,
    out,
    pos,
    vel,
    acc,
    jrk,
    mass,
    ela,
    ids,
    srcs,
    picked,
    near,
    part,
    parts,
    found,
    tb,
    moments,
    in_sems,
    send_sems,
    recv_sems,
    src_send,
    src_recv,
    told,
    beyond,
    *accs,
):
    row = lax.axis_index("row")
    col = lax.axis_index("col")
    stars = pos.shape[1]
    star_tiles = stars // LANES
    blocks = picked.shape[0]
    scale = 1.0 / (stars * rows_n * cols_n)
    waccs, baccs = accs[0::2], accs[1::2]

    loads = [
        pltpu.make_async_copy(src, dst, in_sems.at[i])
        for i, (src, dst) in enumerate(
            zip((ids_h, pos_h, vel_h, acc_h, jrk_h, mass_h, ela_h), (ids, pos, vel, acc, jrk, mass, ela))
        )
    ]
    for load in loads:
        load.start()

    barrier = pltpu.get_barrier_semaphore()
    core = lax.rem(row, 2)
    mate = row + 1 - 2 * core
    reach = cols_n // 4
    near_by = [s * d for d in range(1, reach + 1) for s in (1, -1)]
    pl.semaphore_signal(barrier, 1, device_id={"row": mate}, device_id_type=MESH)
    for d in reversed(near_by):
        pl.semaphore_signal(
            barrier,
            1,
            device_id={"row": row - core + 1, "col": lax.rem(col + d + cols_n, cols_n)},
            device_id_type=MESH,
        )
    for d in range(1, rows_n // 2):
        pl.semaphore_signal(
            barrier, 1, device_id={"row": lax.rem(row - core + 2 * d, rows_n)}, device_id_type=MESH
        )

    loads[0].wait()
    slots = slot_stars(ids, col, cols_n, stars, blocks)
    for load in loads[1:]:
        load.wait()

    t = ela[...]
    p, v, a, j = pos[...], vel[...], acc[...], jrk[...]
    moved_pos = p + t * (v + t * (0.5 * a + t * j / 6.0))
    moved_vel = v + t * (a + 0.5 * t * j)
    own = jnp.concatenate([moved_pos, moved_vel, mass[...]], axis=0)
    srcs[0] = own
    padded = jnp.concatenate([own, jnp.zeros((1, stars), jnp.float32)], axis=0)

    first = (row * cols_n + col) * stars
    mine = []
    for b in range(blocks):
        local = jnp.broadcast_to(slots[b], (8, LANES)) - first
        lane = jnp.bitwise_and(local, LANES - 1)
        tile = jnp.zeros((8, LANES), jnp.float32)
        for s in range(star_tiles):
            held = jnp.logical_and(local >= s * LANES, local < (s + 1) * LANES)
            tile = jnp.where(held, take_lanes(padded[:, s * LANES : (s + 1) * LANES], lane), tile)
        mine.append(tile[0:6])
        picked[b] = tile[0:6]

    def tell_mate():
        pl.semaphore_signal(told, 1, device_id={"row": mate}, device_id_type=MESH)

    def hear(listener, count):
        @pl.when(core == listener)
        def _():
            pl.semaphore_wait(barrier, count)
            tell_mate()

        @pl.when(core != listener)
        def _():
            pl.semaphore_wait(told, 1)

    hear(0, rows_n - 1)

    def send(src, dst, send_sem, recv_sem, axis, peer):
        pltpu.make_async_remote_copy(
            src_ref=src,
            dst_ref=dst,
            send_sem=send_sem,
            recv_sem=recv_sem,
            device_id={axis: peer},
            device_id_type=MESH,
        ).start()

    def whole(ref, send_sem, recv_sem):
        return pltpu.make_async_remote_copy(
            src_ref=ref,
            dst_ref=ref,
            send_sem=send_sem,
            recv_sem=recv_sem,
            device_id={"row": row},
            device_id_type=MESH,
        )

    for d in range(1, rows_n):
        peer = lax.rem(row + d, rows_n)
        send(picked, near.at[d - 1], send_sems.at[0], recv_sems.at[0], "row", peer)
    far_off = [s * d for d in range(reach + 1, cols_n // 2 + 1) for s in (1, -1)][:-1]

    def share():
        def give(d):
            slot = 2 * abs(d) - (1 if d > 0 else 0)
            peer = lax.rem(col + d + cols_n, cols_n)
            send(srcs.at[0], srcs.at[slot], src_send.at[0], src_recv.at[slot - 1], "col", peer)

        hear(1, 2 * len(near_by) + 1)

        @pl.when(core == 1)
        def _():
            for side, d in enumerate((reach, -reach)):
                pl.semaphore_signal(
                    beyond.at[side],
                    1,
                    device_id={"col": lax.rem(col + d + cols_n, cols_n)},
                    device_id_type=MESH,
                )

        for d in near_by:
            give(d)

        @pl.when(core == 1)
        def _():
            pl.semaphore_wait(beyond.at[0], 1)
            pl.semaphore_wait(beyond.at[1], 1)
            tell_mate()

        @pl.when(core != 1)
        def _():
            pl.semaphore_wait(told, 1)

        for d in far_off:
            give(d)

    share()

    sublane = lax.broadcasted_iota(jnp.int32, (8, LANES), 0)
    lane_f = lax.broadcasted_iota(jnp.int32, (8, LANES), 1).astype(jnp.float32)
    for k in range(stars // 8):
        star = first + k * 8 + sublane
        at = jnp.full((8, LANES), -1.0, jnp.float32)
        for b in range(blocks):
            at = jnp.where(jnp.broadcast_to(slots[b], (8, LANES)) == star, lane_f + float(b * LANES), at)
        found[k * 8 : (k + 1) * 8, :] = at
    spots = [
        jnp.max(found[s * LANES : (s + 1) * LANES, :].T, axis=0, keepdims=True).astype(jnp.int32)
        for s in range(star_tiles)
    ]
    moments[32:256, :] = jnp.zeros((224, stars), jnp.bfloat16)
    for unit_acc in accs:
        pltpu.matmul_pop(unit_acc)

    whole(near, send_sems.at[0], recv_sems.at[0]).wait_recv()
    targets = []
    for b in range(blocks):
        total = mine[b]
        for d in range(rows_n - 1):
            total = total + near[d, b]
        targets.append(total)
    spread_targets(targets, tb)

    weigh_block(srcs, 0, tb, moments, waccs, baccs)

    def advance(i, carry):
        whole(srcs.at[0], src_send.at[0], src_recv.at[i - 1]).wait_recv()
        weigh_block(srcs, i, tb, moments, waccs, baccs)
        return carry

    lax.fori_loop(1, cols_n, advance, 0)

    each = LANES // ROWS
    summed = []
    for b in range(blocks):
        direct = folded(waccs[b * each : (b + 1) * each], targets[b])
        bent = folded(baccs[b * each : (b + 1) * each], targets[b])
        summed.append(jnp.concatenate([direct[0:3], direct[3:6] - 3.0 * bent[0:3]], axis=0))
        part[b] = summed[b]
    for d in range(1, rows_n):
        peer = lax.rem(row + d, rows_n)
        send(part, parts.at[d - 1], send_sems.at[1], recv_sems.at[1], "row", peer)
    whole(parts, send_sems.at[1], recv_sems.at[1]).wait_recv()
    forces = []
    for b in range(blocks):
        total = summed[b]
        for d in range(rows_n - 1):
            total = total + parts[d, b]
        forces.append(jnp.concatenate([total * scale, jnp.zeros((2, LANES), jnp.float32)], axis=0))

    for s in range(star_tiles):
        spot = jnp.broadcast_to(spots[s], (8, LANES))
        lane = jnp.bitwise_and(spot, LANES - 1)
        place = jnp.zeros((8, LANES), jnp.float32)
        for b in range(blocks):
            held = jnp.logical_and(spot >= b * LANES, spot < (b + 1) * LANES)
            place = jnp.where(held, take_lanes(forces[b], lane), place)
        lanes = slice(s * LANES, (s + 1) * LANES)
        active = spot[0:3] >= 0
        new_acc, new_jerk = place[0:3], place[3:6]
        new_pos, new_vel = correct(
            pos[:, lanes], vel[:, lanes], acc[:, lanes], jrk[:, lanes], new_acc, new_jerk, ela[:, lanes]
        )
        out[0:3, lanes] = jnp.where(active, new_pos, pos[:, lanes])
        out[4:7, lanes] = jnp.where(active, new_vel, vel[:, lanes])
        out[8:11, lanes] = jnp.where(active, new_acc, acc[:, lanes])
        out[12:15, lanes] = jnp.where(active, new_jerk, jrk[:, lanes])

    whole(near, send_sems.at[0], recv_sems.at[0]).wait_send()
    whole(srcs.at[pl.ds(1, cols_n - 1)], src_send.at[0], src_recv.at[0]).wait_send()
    whole(parts, send_sems.at[1], recv_sems.at[1]).wait_send()


def on_device(rows_n, cols_n, cap, positions, velocities, accels, jerks, masses, elapsed, active_star):
    stars = positions.shape[1]
    groups = rows_n
    size = active_star.shape[0] // groups
    blocks = cap * groups // LANES
    units = blocks * LANES // ROWS
    f32 = jnp.float32
    tiles = (blocks, 6, LANES)

    def kernel(*refs):
        accs = [pltpu.ACC((i // 2) % 2)((ROWS, 256), f32) for i in range(2 * units)]
        pl.run_scoped(functools.partial(step_kernel, rows_n, cols_n, *refs), *accs)

    merged = pl.pallas_call(
        kernel,
        out_shape=pltpu.VMEM((16, stars), f32),
        in_specs=[pl.BlockSpec(memory_space=pltpu.HBM)] * 7,
        out_specs=pl.BlockSpec(memory_space=pltpu.VMEM),
        scratch_shapes=[
            pltpu.VMEM((3, stars), f32),
            pltpu.VMEM((3, stars), f32),
            pltpu.VMEM((3, stars), f32),
            pltpu.VMEM((3, stars), f32),
            pltpu.VMEM((1, stars), f32),
            pltpu.VMEM((1, stars), f32),
            pltpu.VMEM((groups, size), jnp.int32),
            pltpu.VMEM((cols_n, 7, stars), f32),
            pltpu.VMEM(tiles, f32),
            pltpu.VMEM((rows_n - 1,) + tiles, f32),
            pltpu.VMEM(tiles, f32),
            pltpu.VMEM((rows_n - 1,) + tiles, f32),
            pltpu.VMEM((stars, LANES), f32),
            pltpu.VMEM((6, blocks * LANES, LANES), f32),
            pltpu.VMEM((256, stars), jnp.bfloat16),
            pltpu.SemaphoreType.DMA((7,)),
            pltpu.SemaphoreType.DMA((2,)),
            pltpu.SemaphoreType.DMA((2,)),
            pltpu.SemaphoreType.DMA((1,)),
            pltpu.SemaphoreType.DMA((cols_n - 1,)),
            pltpu.SemaphoreType.REGULAR,
            pltpu.SemaphoreType.REGULAR((2,)),
        ],
        compiler_params=pltpu.CompilerParams(
            collective_id=0, has_side_effects=True
        ),
        name="block_step",
    )(
        positions,
        velocities,
        accels,
        jerks,
        masses[None, :],
        elapsed[None, :],
        active_star.reshape(groups, size),
    )
    return tuple(merged[4 * i : 4 * i + 3] for i in range(4))


def solution(mesh):
    split = P(None, ("row", "col"))
    flat = P(("row", "col"))
    return jax.shard_map(
        functools.partial(on_device, mesh.shape["row"], mesh.shape["col"], CAP),
        mesh=mesh,
        in_specs=(split, split, split, split, flat, flat, P()),
        out_specs=(split, split, split, split),
        check_vma=False,
    )
```

```python
import functools
import math

import jax
import jax.numpy as jnp
from jax import lax
from jax.experimental import pallas as pl
from jax.experimental.pallas import tpu as pltpu
from jax.sharding import PartitionSpec as P

softening = 0.001
LANES = 128
MESH = pl.DeviceIdType.MESH
ROWS = 16
CAP = 12


def correct(old_pos, old_vel, old_acc, old_jerk, new_acc, new_jerk, timestep):
    halfstep = 0.5 * timestep
    twelfth = timestep * timestep / 12.0
    new_vel = old_vel + halfstep * (old_acc + new_acc) + twelfth * (old_jerk - new_jerk)
    new_pos = old_pos + halfstep * (old_vel + new_vel) + twelfth * (old_acc - new_acc)
    return (new_pos, new_vel)


def split_moments(block):
    rows = lax.broadcasted_iota(jnp.int32, block.shape, 0)
    weighted = block * jnp.where(rows < 6, block[6:7], 1.0)
    high = weighted.astype(jnp.bfloat16).astype(jnp.float32)
    rest = weighted - high
    middle = rest.astype(jnp.bfloat16).astype(jnp.float32)
    low = rest - middle
    return jnp.concatenate([high, middle, low, jnp.zeros_like(block)], axis=0).astype(jnp.bfloat16)


def below(value):
    return value - value.astype(jnp.bfloat16).astype(jnp.float32)


def weigh_block(srcs, block, tb, moments, waccs, baccs):
    width = srcs.shape[2]
    moments[0:32, :] = split_moments(srcs[block])
    for tile in range(width // 256):
        at = tile * 256
        for unit in range(2):
            pltpu.matmul_push_rhs(
                moments[:, at : at + 256], staging_register=tile % 2, mxu_index=unit, transpose=True
            )
        source = [
            [
                jnp.broadcast_to(srcs[block, k : k + 1, at + h * LANES : at + (h + 1) * LANES], (ROWS, LANES))
                for k in range(6)
            ]
            for h in range(2)
        ]
        for part in range(len(waccs)):
            rows = pl.ds(part * ROWS, ROWS)
            target = [tb[k, rows, :] for k in range(6)]
            weights, bends = [], []
            for h in range(2):
                dx, dy, dz, ux, uy, uz = [source[h][k] - target[k] for k in range(6)]
                radius_sq = (dx * dx + dy * dy) + (dz * dz + softening)
                inverse = lax.rsqrt(radius_sq)
                inverse_sq = inverse * inverse
                weight = inverse * inverse_sq
                closing = (dx * ux + dy * uy) + dz * uz
                weights.append(weight)
                bends.append((weight * inverse_sq) * closing)
            weight = jnp.concatenate(weights, axis=1)
            bend = jnp.concatenate(bends, axis=1)
            fresh = tile % 2 if part < 2 else None
            pltpu.matmul_acc_lhs(waccs[part], weight, load_staged_rhs=fresh)
            pltpu.matmul_acc_lhs(baccs[part], bend)
            pltpu.matmul_acc_lhs(waccs[part], below(weight))
            pltpu.matmul_acc_lhs(baccs[part], below(bend))


def spread_targets(targets, tb):
    for b, tile in enumerate(targets):
        full = jnp.concatenate([tile, jnp.zeros((2, LANES), jnp.float32)], axis=0)
        columns = jnp.concatenate([full] * (LANES // 8), axis=0).T
        for k in range(6):
            tb[k, b * LANES : (b + 1) * LANES, :] = jnp.broadcast_to(columns[:, k : k + 1], (LANES, LANES))


def folded(accs, target):
    turned = jnp.concatenate([pltpu.matmul_pop(acc)[:, 0:LANES] for acc in accs], axis=0).T
    moment = turned[0:8] + turned[8:16] + turned[16:24]
    return moment[0:6] - target * moment[6:7]


def take_lanes(tile, index):
    return jnp.take_along_axis(tile, index, axis=1, mode="promise_in_bounds")


def turn(rows_of):
    return jnp.concatenate([rows_of] * (LANES // rows_of.shape[0]), axis=0).T


def slot_stars(ids, col, cols_n, stars, blocks):
    groups, size = ids.shape
    each = LANES // groups
    turned = turn(ids[...].astype(jnp.float32)).astype(jnp.int32)
    here = jnp.bitwise_and(lax.shift_right_arithmetic(turned, stars.bit_length() - 1), cols_n - 1) == col
    count = jnp.where(here, 1.0, 0.0)
    sub = lax.broadcasted_iota(jnp.int32, (8, LANES), 0)
    before = jnp.zeros((1, LANES), jnp.float32)
    ranks = []
    for i in range(size // 8):
        run = count[i * 8 : (i + 1) * 8]
        for step in (1, 2, 4):
            run = run + jnp.where(sub >= step, pltpu.roll(run, step, 0), 0.0)
        ranks.append(run + before - count[i * 8 : (i + 1) * 8])
        before = before + run[7:8]
    rank = jnp.where(here, jnp.concatenate(ranks, axis=0), -1.0)
    lane = lax.broadcasted_iota(jnp.int32, (1, LANES), 1)
    which = lax.shift_right_arithmetic(lane, groups.bit_length() - 1).astype(jnp.float32)
    found = []
    for b in range(blocks):
        hit = rank == which + float(b * each)
        found.append(jnp.sum(jnp.where(hit, turned + 1, 0), axis=0, keepdims=True) - 1)
    return found


def step_kernel(
    rows_n,
    cols_n,
    pos_h,
    vel_h,
    acc_h,
    jrk_h,
    mass_h,
    ela_h,
    ids_h,
    out,
    pos,
    vel,
    acc,
    jrk,
    mass,
    ela,
    ids,
    srcs,
    picked,
    near,
    part,
    parts,
    found,
    tb,
    moments,
    in_sems,
    send_sems,
    recv_sems,
    src_send,
    src_recv,
    told,
    beyond,
    *accs,
):
    row = lax.axis_index("row")
    col = lax.axis_index("col")
    stars = pos.shape[1]
    star_tiles = stars // LANES
    blocks = picked.shape[0]
    scale = 1.0 / (stars * rows_n * cols_n)
    waccs, baccs = accs[0::2], accs[1::2]

    loads = [
        pltpu.make_async_copy(src, dst, in_sems.at[i])
        for i, (src, dst) in enumerate(
            zip((ids_h, pos_h, vel_h, acc_h, jrk_h, mass_h, ela_h), (ids, pos, vel, acc, jrk, mass, ela))
        )
    ]
    for load in loads:
        load.start()

    barrier = pltpu.get_barrier_semaphore()
    core = lax.rem(row, 2)
    mate = row + 1 - 2 * core
    reach = cols_n // 4
    near_by = [s * d for d in range(1, reach + 1) for s in (1, -1)]
    pl.semaphore_signal(barrier, 1, device_id={"row": mate}, device_id_type=MESH)
    for d in reversed(near_by):
        pl.semaphore_signal(
            barrier,
            1,
            device_id={"row": row - core + 1, "col": lax.rem(col + d + cols_n, cols_n)},
            device_id_type=MESH,
        )
    for d in range(1, rows_n // 2):
        pl.semaphore_signal(
            barrier, 1, device_id={"row": lax.rem(row - core + 2 * d, rows_n)}, device_id_type=MESH
        )

    loads[0].wait()
    slots = slot_stars(ids, col, cols_n, stars, blocks)
    for load in loads[1:]:
        load.wait()

    t = ela[...]
    p, v, a, j = pos[...], vel[...], acc[...], jrk[...]
    moved_pos = p + t * (v + t * (0.5 * a + t * j / 6.0))
    moved_vel = v + t * (a + 0.5 * t * j)
    own = jnp.concatenate([moved_pos, moved_vel, mass[...]], axis=0)
    padded = jnp.concatenate([own, jnp.zeros((1, stars), jnp.float32)], axis=0)
    srcs[0] = padded

    first = (row * cols_n + col) * stars
    mine = []
    for b in range(blocks):
        local = jnp.broadcast_to(slots[b], (8, LANES)) - first
        lane = jnp.bitwise_and(local, LANES - 1)
        tile = jnp.zeros((8, LANES), jnp.float32)
        for s in range(star_tiles):
            held = jnp.logical_and(local >= s * LANES, local < (s + 1) * LANES)
            tile = jnp.where(held, take_lanes(padded[:, s * LANES : (s + 1) * LANES], lane), tile)
        mine.append(tile[0:6])
        picked[b] = tile[0:6]

    def tell_mate():
        pl.semaphore_signal(told, 1, device_id={"row": mate}, device_id_type=MESH)

    def hear(listener, count):
        @pl.when(core == listener)
        def _():
            pl.semaphore_wait(barrier, count)
            tell_mate()

        @pl.when(core != listener)
        def _():
            pl.semaphore_wait(told, 1)

    hear(0, rows_n - 1)

    def send(src, dst, send_sem, recv_sem, axis, peer):
        pltpu.make_async_remote_copy(
            src_ref=src,
            dst_ref=dst,
            send_sem=send_sem,
            recv_sem=recv_sem,
            device_id={axis: peer},
            device_id_type=MESH,
        ).start()

    def whole(ref, send_sem, recv_sem):
        return pltpu.make_async_remote_copy(
            src_ref=ref,
            dst_ref=ref,
            send_sem=send_sem,
            recv_sem=recv_sem,
            device_id={"row": row},
            device_id_type=MESH,
        )

    side = math.isqrt(rows_n // 2)
    y, x = row // (2 * side), lax.rem(row // 2, side)
    steps = sorted(
        ((dy, dx, dc) for dy in range(side) for dx in range(side) for dc in range(2)),
        key=lambda s: (s != (0, 0, 0), -min(s[0], side - s[0]) - min(s[1], side - s[1])),
    )[1:]
    peers = [
        2 * (side * lax.rem(y + dy, side) + lax.rem(x + dx, side)) + lax.rem(core + dc, 2)
        for dy, dx, dc in steps
    ]
    for n, peer in enumerate(peers):
        send(picked, near.at[n], send_sems.at[0], recv_sems.at[0], "row", peer)
    far_off = [s * d for d in range(reach + 1, cols_n // 2 + 1) for s in (1, -1)][:-1]

    def share():
        def give(d):
            slot = 2 * abs(d) - (1 if d > 0 else 0)
            peer = lax.rem(col + d + cols_n, cols_n)
            send(srcs.at[0], srcs.at[slot], src_send.at[0], src_recv.at[slot - 1], "col", peer)

        hear(1, 2 * len(near_by) + 1)

        @pl.when(core == 1)
        def _():
            for side, d in enumerate((reach, -reach)):
                pl.semaphore_signal(
                    beyond.at[side],
                    1,
                    device_id={"col": lax.rem(col + d + cols_n, cols_n)},
                    device_id_type=MESH,
                )

        for d in near_by:
            give(d)

        @pl.when(core == 1)
        def _():
            pl.semaphore_wait(beyond.at[0], 1)
            pl.semaphore_wait(beyond.at[1], 1)
            tell_mate()

        @pl.when(core != 1)
        def _():
            pl.semaphore_wait(told, 1)

        for d in far_off:
            give(d)

    share()

    sublane = lax.broadcasted_iota(jnp.int32, (8, LANES), 0)
    lane_f = lax.broadcasted_iota(jnp.int32, (8, LANES), 1).astype(jnp.float32)
    for k in range(stars // 8):
        star = first + k * 8 + sublane
        at = jnp.full((8, LANES), -1.0, jnp.float32)
        for b in range(blocks):
            at = jnp.where(jnp.broadcast_to(slots[b], (8, LANES)) == star, lane_f + float(b * LANES), at)
        found[k * 8 : (k + 1) * 8, :] = at
    spots = [
        jnp.max(found[s * LANES : (s + 1) * LANES, :].T, axis=0, keepdims=True).astype(jnp.int32)
        for s in range(star_tiles)
    ]
    moments[32:256, :] = jnp.zeros((224, stars), jnp.bfloat16)
    for unit_acc in accs:
        pltpu.matmul_pop(unit_acc)

    whole(near, send_sems.at[0], recv_sems.at[0]).wait_recv()
    targets = []
    for b in range(blocks):
        total = mine[b]
        for d in range(rows_n - 1):
            total = total + near[d, b]
        targets.append(total)
    spread_targets(targets, tb)

    weigh_block(srcs, 0, tb, moments, waccs, baccs)

    def advance(i, carry):
        whole(srcs.at[0], src_send.at[0], src_recv.at[i - 1]).wait_recv()
        weigh_block(srcs, i, tb, moments, waccs, baccs)
        return carry

    lax.fori_loop(1, cols_n, advance, 0)

    each = LANES // ROWS
    summed = []
    for b in range(blocks):
        direct = folded(waccs[b * each : (b + 1) * each], targets[b])
        bent = folded(baccs[b * each : (b + 1) * each], targets[b])
        summed.append(jnp.concatenate([direct[0:3], direct[3:6] - 3.0 * bent[0:3]], axis=0))
        part[b] = summed[b]
    for n, peer in enumerate(peers):
        send(part, parts.at[n], send_sems.at[1], recv_sems.at[1], "row", peer)
    whole(parts, send_sems.at[1], recv_sems.at[1]).wait_recv()
    forces = []
    for b in range(blocks):
        total = summed[b]
        for d in range(rows_n - 1):
            total = total + parts[d, b]
        forces.append(jnp.concatenate([total * scale, jnp.zeros((2, LANES), jnp.float32)], axis=0))

    for s in range(star_tiles):
        spot = jnp.broadcast_to(spots[s], (8, LANES))
        lane = jnp.bitwise_and(spot, LANES - 1)
        place = jnp.zeros((8, LANES), jnp.float32)
        for b in range(blocks):
            held = jnp.logical_and(spot >= b * LANES, spot < (b + 1) * LANES)
            place = jnp.where(held, take_lanes(forces[b], lane), place)
        lanes = slice(s * LANES, (s + 1) * LANES)
        active = spot[0:3] >= 0
        new_acc, new_jerk = place[0:3], place[3:6]
        new_pos, new_vel = correct(
            pos[:, lanes], vel[:, lanes], acc[:, lanes], jrk[:, lanes], new_acc, new_jerk, ela[:, lanes]
        )
        out[0:3, lanes] = jnp.where(active, new_pos, pos[:, lanes])
        out[4:7, lanes] = jnp.where(active, new_vel, vel[:, lanes])
        out[8:11, lanes] = jnp.where(active, new_acc, acc[:, lanes])
        out[12:15, lanes] = jnp.where(active, new_jerk, jrk[:, lanes])

    whole(near, send_sems.at[0], recv_sems.at[0]).wait_send()
    whole(srcs.at[pl.ds(1, cols_n - 1)], src_send.at[0], src_recv.at[0]).wait_send()
    whole(parts, send_sems.at[1], recv_sems.at[1]).wait_send()


def on_device(rows_n, cols_n, cap, positions, velocities, accels, jerks, masses, elapsed, active_star):
    stars = positions.shape[1]
    groups = rows_n
    size = active_star.shape[0] // groups
    blocks = cap * groups // LANES
    units = blocks * LANES // ROWS
    f32 = jnp.float32
    tiles = (blocks, 6, LANES)

    def kernel(*refs):
        accs = [pltpu.ACC((i // 2) % 2)((ROWS, 256), f32) for i in range(2 * units)]
        pl.run_scoped(functools.partial(step_kernel, rows_n, cols_n, *refs), *accs)

    merged = pl.pallas_call(
        kernel,
        out_shape=pltpu.VMEM((16, stars), f32),
        in_specs=[pl.BlockSpec(memory_space=pltpu.HBM)] * 7,
        out_specs=pl.BlockSpec(memory_space=pltpu.VMEM),
        scratch_shapes=[
            pltpu.VMEM((3, stars), f32),
            pltpu.VMEM((3, stars), f32),
            pltpu.VMEM((3, stars), f32),
            pltpu.VMEM((3, stars), f32),
            pltpu.VMEM((1, stars), f32),
            pltpu.VMEM((1, stars), f32),
            pltpu.VMEM((groups, size), jnp.int32),
            pltpu.VMEM((cols_n, 8, stars), f32),
            pltpu.VMEM(tiles, f32),
            pltpu.VMEM((rows_n - 1,) + tiles, f32),
            pltpu.VMEM(tiles, f32),
            pltpu.VMEM((rows_n - 1,) + tiles, f32),
            pltpu.VMEM((stars, LANES), f32),
            pltpu.VMEM((6, blocks * LANES, LANES), f32),
            pltpu.VMEM((256, stars), jnp.bfloat16),
            pltpu.SemaphoreType.DMA((7,)),
            pltpu.SemaphoreType.DMA((2,)),
            pltpu.SemaphoreType.DMA((2,)),
            pltpu.SemaphoreType.DMA((1,)),
            pltpu.SemaphoreType.DMA((cols_n - 1,)),
            pltpu.SemaphoreType.REGULAR,
            pltpu.SemaphoreType.REGULAR((2,)),
        ],
        compiler_params=pltpu.CompilerParams(
            collective_id=0, has_side_effects=True
        ),
        name="block_step",
    )(
        positions,
        velocities,
        accels,
        jerks,
        masses[None, :],
        elapsed[None, :],
        active_star.reshape(groups, size),
    )
    return tuple(merged[4 * i : 4 * i + 3] for i in range(4))


def solution(mesh):
    split = P(None, ("row", "col"))
    flat = P(("row", "col"))
    return jax.shard_map(
        functools.partial(on_device, mesh.shape["row"], mesh.shape["col"], CAP),
        mesh=mesh,
        in_specs=(split, split, split, split, flat, flat, P()),
        out_specs=(split, split, split, split),
        check_vma=False,
    )
```
